32 devices in a mesh: dp: 8 (over z, core), expert: 4 (over y, x).
Axes of the slice: x: 2, y: 2, z: 4, core: 2. Of those that a mesh axis runs over, the one named last changes fastest.
Arguments:
- tokens: bfloat16 [16384, 2048], P(('dp', 'expert')), parts along dimension 0, may hold values from -6 to 6
- modality: int32 [16384], P(('dp', 'expert')), parts along dimension 0, may hold values 0 or 1
- expert_ids: int32 [16384, 2], P(('dp', 'expert')), parts along dimension 0, may hold values from 0 to 3, all different within a row; in each aligned block of 512 rows (0 to 511, 512 to 1023, ...) at most 320 rows name the same one
- route_weights: float32 [16384, 2], P(('dp', 'expert')), parts along dimension 0, may hold values from 0.25 to 1
- norm_gain: float32 [2, 2048], replicated, may hold values from 0.25 to 1.75
- gate_weight: bfloat16 [2048, 3584], P(None, 'expert'), may hold values from -0.125 to 0.125
- up_weight: bfloat16 [2048, 3584], P(None, 'expert'), may hold values from -0.125 to 0.125
- down_weight: bfloat16 [3584, 2048], P('expert'), may hold values from -0.1875 to 0.1875
Outputs:
- mixed: bfloat16 [16384, 2048], P(('dp', 'expert')), parts along dimension 0
The draws below stay inside these ranges and needn't reach their ends.
There are 8 independent parts, one for each index of `dp`. The reference program is written for one: setup_inputs(seed, part) draws one part's arguments, and reference() takes and returns one part's arrays. A program takes and returns all parts, laid end to end along the dimension named above; an argument that names none is the same for every part. Nothing has to cross between parts.
Inputs may be any that keep to these rules, and one draw needn't show every extreme that they name: `expert_ids`: each row names 2 different experts. Among the rows of one device no expert is named by more than 320 rows, a bound that some blocks reach.
All inputs are finite; a program needn't handle non-finite values. No bound on the sum of `modality` on one device may be relied on, other than what follows from the above.
Results may differ from the reference program's by a relative error of at most 0.0054.
Values may be sent and summed in bfloat16 or wider, within the bound.
A program may use at most 128 MiB of HBM per device.

```python
import math
import jax
import jax.numpy as jnp
import numpy as np
from jax import lax

D = 2048
HIDDEN_SIZE = 896
TOP = 2
TOK_DEV = 512
EXPERTS = 4
CAP = 320
TOKENS = 2048
N_EXPERT = 4


def set_ends(result, stream_key, low, largest):
    dims = result.shape
    index_at = [jax.random.randint(jax.random.fold_in(stream_key, axis), (), 0, dims[axis]) for axis in range(len(dims))]
    result = result.at[tuple(index_at)].set(low)
    longest = dims.index(max(dims))
    index_at[longest] = (index_at[longest] + 1) % dims[longest]
    return result.at[tuple(index_at)].set(largest)


def block_scale(own_key, shape, shards, least, high):
    def one(dim, shards_of):
        steps = jax.random.uniform(jax.random.fold_in(jax.random.fold_in(own_key, 6), dim), (shards_of,), jnp.float32, least / len(shards), high / len(shards))
        return jnp.repeat(jnp.exp(steps), shape[dim] // shards_of).reshape((-1,) + (1,) * (len(shape) - dim - 1))

    gain = one(*shards[0])
    for cut in shards[1:]:
        gain = gain * one(*cut)
    return gain


def deal_out(key, own, number, rows, count, top, limit, lean):
    order = jax.random.permutation(key, count)
    heavy_load, ordinary = shares(count, rows * top, limit, lean, True), shares(count, rows * top, limit, lean, False)
    places = jnp.arange(count)

    def named(sizes, offset_by):
        used = int((sizes > 0).sum())
        fixed = max(1, used // 4)
        moved = fixed + (places - fixed + offset_by * (used - fixed)) % max(1, count - fixed)
        return jnp.zeros((count,), jnp.int32).at[order[jnp.where(places < fixed, places, moved)]].set(jnp.asarray(sizes, jnp.int32))

    sizes = jnp.where(number % 4 == 0, named(heavy_load, number // 4), named(ordinary, number - number // 4 - 1))
    mixed = jax.random.permutation(jax.random.fold_in(own, 3), count)
    source_of, taker = mixed[0:count // 2 * 2:2], mixed[1:count // 2 * 2:2]
    room = jnp.minimum(sizes[source_of] - 1, limit - sizes[taker]) // 2
    room = jnp.where((source_of == order[0]) | (taker == order[0]) | (sizes[taker] == 0), 0, jnp.maximum(room, 0))
    moved = jax.random.randint(jax.random.fold_in(own, 4), (count // 2,), 0, 1 << 20) % (room + 1)
    sizes = sizes.at[source_of].add(-moved).at[taker].add(moved)
    labels = jnp.searchsorted(jnp.cumsum(sizes), jnp.arange(rows * top), side="right").astype(jnp.int32)
    table = labels.reshape(top, rows).T
    table = table[jax.random.permutation(jax.random.fold_in(own, 1), rows)]
    offset_by = jax.random.randint(jax.random.fold_in(own, 2), (rows, 1), 0, top)
    return jnp.take_along_axis(table, (jnp.arange(top)[None, :] + offset_by) % top, axis=1)


def shares(number_of, total, bound, slope, full):
    loads = [(1 << 20) // math.isqrt(rank ** slope) + 1 for rank in range(1, number_of + 1)]
    largest = bound if full else min(bound, max(-(-total // number_of), total * loads[0] // sum(loads)))
    least = 1 if total - largest >= number_of - 1 else 0
    counts, rest = [largest] + [least] * (number_of - 1), total - largest - least * (number_of - 1)
    while rest > 0:
        free = [i for i in range(1, number_of) if counts[i] < largest] or [i for i in range(1, number_of) if counts[i] < bound]
        pool, budget = sum([loads[i] for i in free]), rest
        for i in free:
            extra = min(bound - counts[i], max(1, budget * loads[i] // pool), rest)
            counts[i] = counts[i] + extra
            rest = rest - extra
    return np.array(counts)


def bell_draw(stream_key, shape, spread, most, split=(), held_as=jnp.bfloat16):
    factor_of = block_scale(stream_key, shape, split, -0.22, 0.18) if split else 1.0
    result = jax.random.normal(stream_key, shape, jnp.float32) * spread * factor_of
    return jnp.minimum(jnp.maximum(result, -most), most).astype(held_as)


def setup_inputs(seed: int = 0, part: int = 0) -> dict:
    key_list = jax.random.split(jax.random.key(seed), 9)
    part_splits = jax.random.split(jax.random.fold_in(key_list[8], part), 9)
    tokens = bell_draw(part_splits[0], (TOKENS, D), 1.0, 6.0, ((0, 4),))
    modality = set_ends((jax.random.randint(part_splits[1], (TOKENS,), 0, 2) < 1).astype(jnp.int32), jax.random.fold_in(part_splits[1], 1), 0, 1)
    expert_ids_keys = jax.random.split(jax.random.fold_in(part_splits[2], 1), TOKENS // TOK_DEV)
    expert_ids_turns = jax.random.permutation(jax.random.fold_in(part_splits[2], 3), TOKENS // TOK_DEV)
    expert_ids = jax.vmap(lambda own, number: deal_out(jax.random.fold_in(part_splits[2], 2), own, number, TOK_DEV, EXPERTS, TOP, CAP, 1))(expert_ids_keys, expert_ids_turns).reshape((TOKENS, TOP))
    route_weights = jnp.clip(0.25 + 0.75 * jax.random.uniform(part_splits[3], (TOKENS, TOP), jnp.float32) ** block_scale(part_splits[3], (TOKENS, TOP), ((0, 4),), -0.2, 0.2), 0.25, 1.0)
    norm_gain = jnp.clip(1.0 + 0.15 * jax.random.normal(key_list[4], (2, D), jnp.float32), 0.25, 1.75)
    gate_weight = bell_draw(key_list[5], (D, EXPERTS * HIDDEN_SIZE), D ** -0.5, 0.125, ((1, 4),))
    up_weight = bell_draw(key_list[6], (D, EXPERTS * HIDDEN_SIZE), D ** -0.5, 0.125, ((1, 4),))
    down_weight = bell_draw(key_list[7], (EXPERTS * HIDDEN_SIZE, D), HIDDEN_SIZE ** -0.5, 0.1875, ((0, 4),))
    return dict(tokens=tokens, modality=modality, expert_ids=expert_ids, route_weights=route_weights, norm_gain=norm_gain, gate_weight=gate_weight, up_weight=up_weight, down_weight=down_weight)


epsilon = 1e-05

def normalize(tokens, modality, norm_gain):
    values = tokens.astype(jnp.float32)
    square = lax.optimization_barrier(jnp.mean(values * values, axis=1, keepdims=True))
    gains = jnp.where(modality[:, None] == 1, norm_gain[1][None, :], norm_gain[0][None, :])
    return (values * lax.rsqrt(square + epsilon) * gains).astype(jnp.bfloat16)

def slot_table(expert_ids, experts, capacity):
    fanout = expert_ids.shape[1]
    flat_ids = expert_ids.reshape(-1).astype(jnp.int32)
    columns = jnp.arange(experts, dtype=jnp.int32)
    onehot = (flat_ids[:, None] == columns[None, :]).astype(jnp.int32)
    earlier = jnp.cumsum(onehot, axis=0).astype(jnp.int32) - onehot
    position = lax.optimization_barrier(jnp.sum(earlier * onehot, axis=1)).astype(jnp.int32)
    slots = (flat_ids * capacity + position).astype(jnp.int32)
    sources = (jnp.arange(flat_ids.shape[0], dtype=jnp.int32) // fanout).astype(jnp.int32)
    owners = jnp.full((experts * capacity,), -1, jnp.int32).at[slots].set(sources)
    return (slots, owners)

def pack_rows(normed, owners):
    chosen = jnp.take(normed, jnp.maximum(owners, 0), axis=0)
    return jnp.where(owners[:, None] >= 0, chosen, jnp.zeros_like(chosen))

def expert_rows(rows, gate_cols, up_cols, down_rows):
    gate = jnp.dot(rows, gate_cols, preferred_element_type=jnp.float32)
    upper = jnp.dot(rows, up_cols, preferred_element_type=jnp.float32)
    active = (jax.nn.silu(gate) * upper).astype(jnp.bfloat16)
    return jnp.dot(active, down_rows, preferred_element_type=jnp.float32)

def reference(tokens, modality, expert_ids, route_weights, norm_gain, gate_weight, up_weight, down_weight):
    normed = normalize(tokens, modality, norm_gain)
    block_normed = normed.reshape(N_EXPERT, TOK_DEV, D)
    block_ids = expert_ids.reshape(N_EXPERT, TOK_DEV, TOP)
    slots, owners = jax.vmap(lambda ids: slot_table(ids, EXPERTS, CAP))(block_ids)
    packed = jax.vmap(pack_rows)(block_normed, owners)
    per_expert = packed.reshape(N_EXPERT, EXPERTS, CAP, D).transpose(1, 0, 2, 3).reshape(EXPERTS, N_EXPERT * CAP, D)

    def run_one(index):
        start = (index * HIDDEN_SIZE).astype(jnp.int32)
        gate_cols = lax.dynamic_slice_in_dim(gate_weight, start, HIDDEN_SIZE, 1)
        up_cols = lax.dynamic_slice_in_dim(up_weight, start, HIDDEN_SIZE, 1)
        down_rows = lax.dynamic_slice_in_dim(down_weight, start, HIDDEN_SIZE, 0)
        rows = lax.dynamic_index_in_dim(per_expert, index, 0, keepdims=False)
        return expert_rows(rows, gate_cols, up_cols, down_rows).astype(jnp.bfloat16)
    outputs = lax.map(run_one, jnp.arange(EXPERTS, dtype=jnp.int32))
    by_block = outputs.reshape(EXPERTS, N_EXPERT, CAP, D).transpose(1, 0, 2, 3).reshape(N_EXPERT, EXPERTS * CAP, D)
    picked = jax.vmap(lambda table, where_to: jnp.take(table, where_to, axis=0))(by_block, slots)
    picked = picked.reshape(TOKENS, TOP, D).astype(jnp.float32)
    mixed = tokens.astype(jnp.float32) + lax.optimization_barrier(jnp.sum(route_weights[:, :, None] * picked, axis=1))
    return mixed.astype(jnp.bfloat16)
```

```python
import functools

import jax
import jax.numpy as jnp
from jax import lax
from jax.experimental import pallas as pl
from jax.experimental.pallas import tpu as pltpu
from jax.sharding import PartitionSpec as P

epsilon = 1e-05
LANES = 128
AXIS = "expert"


def grid_side(devices):
    side = 1
    while side * side < devices:
        side += 1
    return side if side * side == devices else devices


def moe_kernel(
    devices,
    tokens_hbm,
    modality_ref,
    ids_ref,
    weights_ref,
    gain_ref,
    gate_hbm,
    up_hbm,
    down_hbm,
    out_ref,
    tokens,
    gate,
    up,
    down,
    normed,
    total,
    place_rows,
    place_cols,
    share_cols,
    packed,
    arrived,
    finished,
    returned,
    load_sem,
    go_send,
    go_recv,
    back_send,
    back_recv,
):
    waves, _, chunk, width = packed.shape
    tok_rows = tokens.shape[0]
    fanout = ids_ref.shape[0]
    me = lax.axis_index(AXIS)
    side = grid_side(devices)
    mine_hi, mine_lo = me // side, me % side
    lines = devices // side

    def ahead(step):
        return ((mine_hi + step // side) % lines) * side + (mine_lo + step % side) % side

    def behind(step):
        return ((mine_hi + lines - step // side) % lines) * side + (
            mine_lo + side - step % side
        ) % side

    def go(wave, step):
        return pltpu.make_async_remote_copy(
            src_ref=packed.at[wave, step],
            dst_ref=arrived.at[wave, step],
            send_sem=go_send.at[wave, step],
            recv_sem=go_recv.at[wave, step],
            device_id={AXIS: ahead(step)},
            device_id_type=pl.DeviceIdType.MESH,
        )

    def back(wave, step):
        return pltpu.make_async_remote_copy(
            src_ref=finished.at[wave, step],
            dst_ref=returned.at[wave, step],
            send_sem=back_send.at[wave, step],
            recv_sem=back_recv.at[wave, step],
            device_id={AXIS: behind(step)},
            device_id_type=pl.DeviceIdType.MESH,
        )

    loads = [
        pltpu.make_async_copy(tokens_hbm, tokens, load_sem.at[0]),
        pltpu.make_async_copy(gate_hbm, gate, load_sem.at[1]),
        pltpu.make_async_copy(up_hbm, up, load_sem.at[2]),
        pltpu.make_async_copy(down_hbm, down, load_sem.at[3]),
    ]
    for load in loads:
        load.start()

    barrier = pltpu.get_barrier_semaphore()

    def greet(step, carry):
        pl.semaphore_signal(
            barrier, inc=1, device_id={AXIS: ahead(step)}, device_id_type=pl.DeviceIdType.MESH
        )
        return carry

    lax.fori_loop(1, devices, greet, 0)

    expert = lax.broadcasted_iota(jnp.int32, (LANES, tok_rows), 0)
    named = jnp.zeros((LANES, tok_rows), jnp.float32)
    share = jnp.zeros((LANES, tok_rows), jnp.float32)
    for k in range(fanout):
        hit = expert == ids_ref[k : k + 1, :]
        named = jnp.where(hit, 1.0, named)
        share = jnp.where(hit, weights_ref[k : k + 1, :], share)
    before = (
        lax.broadcasted_iota(jnp.int32, (tok_rows, tok_rows), 0)
        < lax.broadcasted_iota(jnp.int32, (tok_rows, tok_rows), 1)
    )
    count = jnp.dot(
        named.astype(jnp.bfloat16),
        jnp.where(before, 1.0, 0.0).astype(jnp.bfloat16),
        preferred_element_type=jnp.float32,
    )
    place = jnp.where(named > 0.5, count, -1.0)
    place_rows[...] = place
    place_cols[...] = place.T
    share_cols[...] = share.T
    image = jnp.broadcast_to(modality_ref[...].astype(jnp.float32), (LANES, tok_rows)).T

    loads[0].wait()
    rows = 64
    for start in range(0, tok_rows, rows):
        values = tokens[start : start + rows, :].astype(jnp.float32)
        square = jnp.mean(values * values, axis=1, keepdims=True)
        gains = jnp.where(
            image[start : start + rows, :1] > 0.5, gain_ref[1:2, :], gain_ref[0:1, :]
        )
        normed[start : start + rows, :] = (
            values * lax.rsqrt(square + epsilon) * gains
        ).astype(jnp.bfloat16)

    def pack(wave, step, target):
        line = place_rows[pl.ds(ahead(step), 1), :]
        slot = lax.broadcasted_iota(jnp.int32, (chunk, tok_rows), 0) + wave * chunk
        pick = jnp.where(line == slot.astype(jnp.float32), 1.0, 0.0).astype(jnp.bfloat16)
        target[wave, step] = jnp.dot(
            pick, normed[...], preferred_element_type=jnp.float32
        ).astype(jnp.bfloat16)

    others = devices - 1
    items = waves * others

    def which(item):
        return item // others, others - item % others

    pl.semaphore_wait(barrier, others)

    def send(item, carry):
        wave, step = which(item)
        pack(wave, step, packed)
        go(wave, step).start()
        return carry

    lax.fori_loop(0, items, send, 0)

    for load in loads[1:]:
        load.wait()

    def feed(source, target, wave, step):
        value = source[wave, step]
        opened = jnp.dot(value, gate[...], preferred_element_type=jnp.float32)
        upper = jnp.dot(value, up[...], preferred_element_type=jnp.float32)
        active = (opened / (1.0 + jnp.exp(-opened)) * upper).astype(jnp.bfloat16)
        target[wave, step] = jnp.dot(
            active, down[...], preferred_element_type=jnp.float32
        ).astype(jnp.bfloat16)

    def spread(wave, step):
        lane = lax.broadcasted_iota(jnp.int32, (tok_rows, LANES), 1) == ahead(step)
        line = jnp.sum(jnp.where(lane, place_cols[...], 0.0), axis=1, keepdims=True)
        worth = jnp.sum(jnp.where(lane, share_cols[...], 0.0), axis=1, keepdims=True)
        slot = lax.broadcasted_iota(jnp.int32, (tok_rows, chunk), 1) + wave * chunk
        spots = jnp.where(line == slot.astype(jnp.float32), worth, 0.0)
        high = spots.astype(jnp.bfloat16)
        low = (spots - high.astype(jnp.float32)).astype(jnp.bfloat16)
        value = returned[wave, step]
        return jnp.dot(high, value, preferred_element_type=jnp.float32) + jnp.dot(
            low, value, preferred_element_type=jnp.float32
        )

    total[...] = tokens[...].astype(jnp.float32)

    def local(wave, carry):
        pack(wave, 0, arrived)
        feed(arrived, returned, wave, 0)
        total[...] += spread(wave, 0)
        return carry

    lax.fori_loop(0, waves, local, 0)

    def serve(item, carry):
        wave, step = which(item)
        go(wave, step).wait_recv()
        feed(arrived, finished, wave, step)
        back(wave, step).start()
        return carry

    lax.fori_loop(0, items, serve, 0)

    def collect(item, carry):
        wave, step = which(item)
        back(wave, step).wait_recv()
        total[...] += spread(wave, step)
        return carry

    lax.fori_loop(0, items - 1, collect, 0)
    wave, step = which(items - 1)
    back(wave, step).wait_recv()
    out_ref[...] = (total[...] + spread(wave, step)).astype(out_ref.dtype)

    def settle(item, carry):
        wave, step = which(item)
        go(wave, step).wait_send()
        back(wave, step).wait_send()
        return carry

    lax.fori_loop(0, items, settle, 0)


def pair_kernel(
    blocks,
    groups,
    pieces,
    tokens_hbm,
    modality_hbm,
    ids_hbm,
    weights_hbm,
    gain_hbm,
    gate_hbm,
    up_hbm,
    down_hbm,
    out_ref,
    modality_ref,
    ids_ref,
    weights_ref,
    gain_ref,
    tokens,
    sorted_tokens,
    near_tokens,
    gate,
    up,
    down,
    far_gate,
    far_up,
    far_down,
    normed,
    near_normed,
    total,
    near_total,
    facts,
    sorted_facts,
    near_facts,
    slots,
    columns,
    sum_out,
    sum_in,
    load_sem,
    facts_sem,
    dense_send,
    dense_recv,
    sum_send,
    sum_recv,
    wide_send,
    wide_recv,
    tall_send,
    tall_recv,
):
    tok_rows, width = tokens.shape
    hidden = gate.shape[1]
    fanout = ids_ref.shape[0]
    devices = lax.axis_size(AXIS)
    capacity = tok_rows * fanout * 5 // (4 * devices)
    part = tok_rows // blocks
    free = (tok_rows - capacity) // part
    me = lax.axis_index(AXIS)
    copy_of = lax.axis_index("dp")
    layer, core = copy_of // 2, copy_of % 2
    beside = me // 2 * 2 + 1 - me % 2
    above = (1 - me // 2) * 2 + me % 2
    diagonal = (1 - me // 2) * 2 + 1 - me % 2
    other_layer = (layer // 2 * 2 + 1 - layer % 2) * 2 + core
    other_core = layer * 2 + 1 - core
    quarter = layer % 2 * 2 + core
    layer_quarter = (1 - layer % 2) * 2 + core

    def remote(source, target, send_sem, recv_sem, copy, peer):
        return pltpu.make_async_remote_copy(
            src_ref=source,
            dst_ref=target,
            send_sem=send_sem,
            recv_sem=recv_sem,
            device_id={"dp": copy, AXIS: peer},
            device_id_type=pl.DeviceIdType.MESH,
        )

    def part_rows(block):
        return pl.ds(pl.multiple_of(block * part, part), part)

    def dense(block):
        rows = part_rows(block)
        return remote(
            sorted_tokens.at[rows],
            near_tokens.at[rows],
            dense_send.at[block],
            dense_recv.at[block],
            copy_of,
            beside,
        )

    def sums(block):
        rows = part_rows(block)
        return remote(
            sum_out.at[rows], sum_in.at[rows], sum_send.at[block], sum_recv.at[block], copy_of, beside
        )

    wide_rows = width // 4 // groups
    tall_rows = hidden // 4 // pieces

    def weight_copy(stage, kind, index):
        if kind < 2:
            near, far = ((gate_hbm, far_gate), (up_hbm, far_up))[kind]
            count, whole, send, recv = wide_rows, width // 4, wide_send.at[kind], wide_recv.at[kind]
        else:
            near, far = down_hbm, far_down
            count, whole, send, recv = tall_rows, hidden // 4, tall_send, tall_recv
        which = layer_quarter if stage == 3 else quarter
        rows = pl.ds(pl.multiple_of(which * whole + index * count, count), count)
        copy, peer = ((copy_of, above), (other_layer, me), (other_core, me), (other_core, me))[stage]
        return remote(
            (near if stage == 0 else far).at[rows],
            far.at[rows],
            send.at[stage, index],
            recv.at[stage, index],
            copy,
            peer,
        )

    def arrived_across(kind, index):
        weight_copy(0, kind, index).wait_recv()
        weight_copy(1, kind, index).start()
        weight_copy(2, kind, index).start()

    def arrived_along(kind, index):
        weight_copy(1, kind, index).wait_recv()
        weight_copy(3, kind, index).start()

    def each(count, step, start=0):
        def body(index, carry):
            step(index)
            return carry

        lax.fori_loop(start, count, body, 0)

    loads = [
        pltpu.make_async_copy(source, target, load_sem.at[index])
        for index, (source, target) in enumerate(
            (
                (ids_hbm, ids_ref),
                (weights_hbm, weights_ref),
                (modality_hbm, modality_ref),
                (tokens_hbm, tokens),
                (gain_hbm, gain_ref),
                (gate_hbm, gate),
                (up_hbm, up),
                (down_hbm, down),
            )
        )
    ]
    for load in loads[:5]:
        load.start()
    barrier = pltpu.get_barrier_semaphore()
    for copy, peer in ((copy_of, beside), (copy_of, above), (other_layer, me), (other_core, me)):
        pl.semaphore_signal(
            barrier,
            inc=1,
            device_id={"dp": copy, AXIS: peer},
            device_id_type=pl.DeviceIdType.MESH,
        )
    for load in loads[:3]:
        load.wait()

    lines = 8
    expert = lax.broadcasted_iota(jnp.int32, (lines, tok_rows), 0)
    named = jnp.zeros((lines, tok_rows), jnp.float32)
    share = jnp.where(
        expert == devices,
        jnp.broadcast_to(modality_ref[...].astype(jnp.float32), (lines, tok_rows)),
        0.0,
    )
    late = jnp.zeros((1, tok_rows), jnp.float32)
    for k in range(fanout):
        share = jnp.where(expert == ids_ref[k : k + 1, :], weights_ref[k : k + 1, :], share)
        late = jnp.where(ids_ref[k : k + 1, :] == diagonal, 1.0, late)
    facts[...] = share
    named = jnp.where(expert == 0, late, 1.0 - late)
    before = (
        lax.broadcasted_iota(jnp.int32, (tok_rows, tok_rows), 0)
        < lax.broadcasted_iota(jnp.int32, (tok_rows, tok_rows), 1)
    )
    count = jnp.dot(
        named.astype(jnp.bfloat16),
        jnp.where(before, 1.0, 0.0).astype(jnp.bfloat16),
        preferred_element_type=jnp.float32,
    )
    slots[...] = jnp.broadcast_to(
        jnp.where(late > 0.5, tok_rows - 1.0 - count[0:1, :], count[1:2, :]), (lines, tok_rows)
    )

    def sort(block):
        slot = lax.broadcasted_iota(jnp.int32, (part, tok_rows), 0) + block * part
        pick = jnp.where(slots[0:1, :] == slot.astype(jnp.float32), 1.0, 0.0).astype(jnp.bfloat16)
        sorted_tokens[part_rows(block)] = jnp.dot(
            pick, tokens[...], preferred_element_type=jnp.float32
        ).astype(jnp.bfloat16)

    loads[3].wait()
    for load in loads[5:]:
        load.start()
    sort(0)
    pl.semaphore_wait(barrier, 4)
    dense(0).start()
    each(groups, lambda index: [weight_copy(0, kind, index).start() for kind in range(2)])
    each(pieces, lambda index: weight_copy(0, 2, index).start())

    def leave(block):
        sort(block)
        dense(block).start()

    each(blocks, leave, 1)

    def keep(place, line):
        columns[place] = jnp.broadcast_to(line, (LANES, tok_rows)).T

    own_mine, own_far, near_mine, near_far, near_image, own_image, own_slot = range(7)
    keep(own_slot, slots[0:1, :])
    keep(own_mine, facts[pl.ds(me, 1), :])
    keep(own_far, facts[pl.ds(above, 1), :])
    keep(own_image, facts[devices : devices + 1, :])

    def places(start, count):
        slot = lax.broadcasted_iota(jnp.int32, (tok_rows, count), 1) + start
        here = columns[own_slot, :, 0:1] == slot.astype(jnp.float32)
        return jnp.where(here, 1.0, 0.0).astype(jnp.bfloat16)

    coarse = share.astype(jnp.bfloat16)
    fine = (share - coarse.astype(jnp.float32)).astype(jnp.bfloat16)
    every = places(0, tok_rows)
    sorted_facts[...] = jnp.dot(coarse, every, preferred_element_type=jnp.float32) + jnp.dot(
        fine, every, preferred_element_type=jnp.float32
    )
    told = remote(sorted_facts, near_facts, facts_sem.at[0], facts_sem.at[1], copy_of, beside)
    told.start()

    def normalize(source, target, image, rows):
        values = source[rows, :].astype(jnp.float32)
        square = jnp.mean(values * values, axis=1, keepdims=True)
        gains = jnp.where(image > 0.5, gain_ref[1:2, :], gain_ref[0:1, :])
        target[rows, :] = (values * lax.rsqrt(square + epsilon) * gains).astype(jnp.bfloat16)

    def feed(value, opening, upping, closing):
        opened = jnp.dot(value, opening[...], preferred_element_type=jnp.float32)
        upper = jnp.dot(value, upping[...], preferred_element_type=jnp.float32)
        active = (opened / (1.0 + jnp.exp(-opened)) * upper).astype(jnp.bfloat16)
        result = jnp.dot(active, closing[...], preferred_element_type=jnp.float32)
        return result.astype(jnp.bfloat16).astype(jnp.float32)

    loads[4].wait()
    rows = 64

    def ready(index):
        here = pl.ds(pl.multiple_of(index * rows, rows), rows)
        normalize(tokens, normed, columns[own_image, here, 0:1], here)

    each(tok_rows // rows, ready)
    for load in loads[5:]:
        load.wait()

    batch = tok_rows // groups

    def batch_rows(group):
        return pl.ds(pl.multiple_of(group * batch, batch), batch)

    told.wait_recv()
    keep(near_mine, near_facts[pl.ds(me, 1), :])
    keep(near_far, near_facts[pl.ds(above, 1), :])
    keep(near_image, near_facts[devices : devices + 1, :])

    def both(group):
        here = batch_rows(group)
        total[here, :] = tokens[here, :].astype(jnp.float32) + columns[own_mine, here, 0:1] * feed(
            normed[here, :], gate, up, down
        )
        arrived_across(0, group)

        @pl.when(group > 0)
        def _():
            arrived_along(1, group - 1)

        arrived_across(1, group)
        for index in range(blocks // groups):
            dense(group * (blocks // groups) + index).wait_recv()
        for start in range(0, batch, rows):
            few = pl.ds(pl.multiple_of(group * batch + start, rows), rows)
            normalize(near_tokens, near_normed, columns[near_image, few, 0:1], few)
        near = columns[near_mine, here, 0:1] * feed(near_normed[here, :], gate, up, down)
        near_total[here, :] = near
        sum_out[here, :] = near.astype(jnp.bfloat16)
        for index in range(blocks // groups):
            block = group * (blocks // groups) + index

            @pl.when(block < free)
            def _():
                sums(block).start()

        arrived_along(0, group)

    each(groups, both)

    def close(index):
        arrived_across(2, index)

        @pl.when(index == 0)
        def _():
            arrived_along(1, groups - 1)

        @pl.when(index > 0)
        def _():
            arrived_along(2, index - 1)

    each(pieces, close)
    arrived_along(2, pieces - 1)

    def joined(kind, index):
        weight_copy(2, kind, index).wait_recv()
        weight_copy(3, kind, index).wait_recv()

    each(groups, lambda index: [joined(kind, index) for kind in range(2)])
    each(pieces, lambda index: joined(2, index))

    def finish(block):
        here = part_rows(block)
        near = near_total[here, :] + columns[near_far, here, 0:1] * feed(
            near_normed[here, :], far_gate, far_up, far_down
        )
        sum_out[here, :] = near.astype(jnp.bfloat16)
        sums(block).start()

    each(blocks, finish, free)

    def own(group):
        here = batch_rows(group)
        total[here, :] += columns[own_far, here, 0:1] * feed(
            normed[here, :], far_gate, far_up, far_down
        )

    each(groups, own)

    def take(block):
        sums(block).wait_recv()
        return jnp.dot(
            places(block * part, part), sum_in[part_rows(block)], preferred_element_type=jnp.float32
        )

    def collect(block):
        total[...] += take(block)

    each(blocks - 1, collect)
    out_ref[...] = (total[...] + take(blocks - 1)).astype(out_ref.dtype)

    told.wait_send()
    each(blocks, lambda block: dense(block).wait_send())
    each(blocks, lambda block: sums(block).wait_send())

    def sent(kind, index):
        for stage in range(4):
            weight_copy(stage, kind, index).wait_send()

    each(groups, lambda index: [sent(kind, index) for kind in range(2)])
    each(pieces, lambda index: sent(2, index))


def pair_scratch(tok_rows, width, hidden, fanout, blocks, groups, pieces):
    dense = pltpu.VMEM((tok_rows, width), jnp.bfloat16)
    sums = pltpu.VMEM((tok_rows, width), jnp.float32)
    facts = pltpu.VMEM((8, tok_rows), jnp.float32)
    wide = pltpu.VMEM((width, hidden), jnp.bfloat16)
    tall = pltpu.VMEM((hidden, width), jnp.bfloat16)
    by_block = pltpu.SemaphoreType.DMA((blocks,))
    by_group = pltpu.SemaphoreType.DMA((2, 4, groups))
    by_piece = pltpu.SemaphoreType.DMA((4, pieces))
    return [
        pltpu.VMEM((1, tok_rows), jnp.int32), pltpu.VMEM((fanout, tok_rows), jnp.int32),
        pltpu.VMEM((fanout, tok_rows), jnp.float32), pltpu.VMEM((2, width), jnp.float32),
        dense, dense, dense, wide, wide, tall, wide, wide, tall, dense, dense, sums, sums,
        facts, facts, facts, facts, pltpu.VMEM((7, tok_rows, LANES), jnp.float32), dense, dense,
        pltpu.SemaphoreType.DMA((8,)), pltpu.SemaphoreType.DMA((2,)),
        by_block, by_block, by_block, by_block, by_group, by_group, by_piece, by_piece,
    ]


def direct_scratch(tok_rows, width, hidden, buffer, sems):
    return [
        pltpu.VMEM((tok_rows, width), jnp.bfloat16),
        pltpu.VMEM((width, hidden), jnp.bfloat16),
        pltpu.VMEM((width, hidden), jnp.bfloat16),
        pltpu.VMEM((hidden, width), jnp.bfloat16),
        pltpu.VMEM((tok_rows, width), jnp.bfloat16),
        pltpu.VMEM((tok_rows, width), jnp.float32),
        pltpu.VMEM((LANES, tok_rows), jnp.float32),
        pltpu.VMEM((tok_rows, LANES), jnp.float32),
        pltpu.VMEM((tok_rows, LANES), jnp.float32),
        buffer,
        buffer,
        buffer,
        buffer,
        pltpu.SemaphoreType.DMA((4,)),
        sems,
        sems,
        sems,
        sems,
    ]


def shards(
    tokens, modality, expert_ids, route_weights, norm_gain, gate_weight, up_weight, down_weight
):
    devices = lax.axis_size(AXIS)
    tok_rows, width = tokens.shape
    fanout = expert_ids.shape[1]
    hidden = gate_weight.shape[1]
    capacity = min(tok_rows, tok_rows * fanout * 5 // (4 * devices))
    waves = 2 if capacity % 32 == 0 and capacity >= 256 else 1
    chunk = capacity // waves
    buffer = pltpu.VMEM((waves, devices, chunk, width), jnp.bfloat16)
    near = pl.BlockSpec(memory_space=pltpu.VMEM)
    far = pl.BlockSpec(memory_space=pl.ANY)
    sems = pltpu.SemaphoreType.DMA((waves, devices))
    blocks, groups, pieces = 8, 4, hidden // 128
    paired = (
        devices == 4
        and lax.axis_size("dp") % 4 == 0
        and tok_rows % (LANES * groups) == 0
        and tok_rows % (64 * blocks) == 0
        and width % (64 * groups) == 0
        and hidden % 128 == 0
    )
    if paired:
        kernel = functools.partial(pair_kernel, blocks, groups, pieces)
        scratch = pair_scratch(tok_rows, width, hidden, fanout, blocks, groups, pieces)
    else:
        kernel = functools.partial(moe_kernel, devices)
        scratch = direct_scratch(tok_rows, width, hidden, buffer, sems)
    return pl.pallas_call(
        kernel,
        out_shape=pltpu.VMEM((tok_rows, width), jnp.bfloat16),
        in_specs=[far] + [far if paired else near] * 4 + [far] * 3,
        out_specs=near,
        scratch_shapes=scratch,
        compiler_params=pltpu.CompilerParams(
            collective_id=0, has_side_effects=True, vmem_limit_bytes=(60 if paired else 58) * 1024 * 1024
        ),
    )(
        tokens,
        modality.reshape(1, tok_rows),
        expert_ids.T,
        route_weights.T,
        norm_gain,
        gate_weight,
        up_weight,
        down_weight,
    )


def solution(mesh):
    placed = (
        P(("dp", AXIS), None),
        P(("dp", AXIS)),
        P(("dp", AXIS), None),
        P(("dp", AXIS), None),
        P(),
        P(None, AXIS),
        P(None, AXIS),
        P(AXIS, None),
    )
    return jax.shard_map(
        shards, mesh=mesh, in_specs=placed, out_specs=P(("dp", AXIS), None), check_vma=False
    )
```

```python
import functools

import jax
import jax.numpy as jnp
from jax import lax
from jax.experimental import pallas as pl
from jax.experimental.pallas import tpu as pltpu
from jax.sharding import PartitionSpec as P

epsilon = 1e-05
LANES = 128
AXIS = "expert"


def grid_side(devices):
    side = 1
    while side * side < devices:
        side += 1
    return side if side * side == devices else devices


def moe_kernel(
    devices,
    tokens_hbm,
    modality_ref,
    ids_ref,
    weights_ref,
    gain_ref,
    gate_hbm,
    up_hbm,
    down_hbm,
    out_ref,
    tokens,
    gate,
    up,
    down,
    normed,
    total,
    place_rows,
    place_cols,
    share_cols,
    packed,
    arrived,
    finished,
    returned,
    load_sem,
    go_send,
    go_recv,
    back_send,
    back_recv,
):
    waves, _, chunk, width = packed.shape
    tok_rows = tokens.shape[0]
    fanout = ids_ref.shape[0]
    me = lax.axis_index(AXIS)
    side = grid_side(devices)
    mine_hi, mine_lo = me // side, me % side
    lines = devices // side

    def ahead(step):
        return ((mine_hi + step // side) % lines) * side + (mine_lo + step % side) % side

    def behind(step):
        return ((mine_hi + lines - step // side) % lines) * side + (
            mine_lo + side - step % side
        ) % side

    def go(wave, step):
        return pltpu.make_async_remote_copy(
            src_ref=packed.at[wave, step],
            dst_ref=arrived.at[wave, step],
            send_sem=go_send.at[wave, step],
            recv_sem=go_recv.at[wave, step],
            device_id={AXIS: ahead(step)},
            device_id_type=pl.DeviceIdType.MESH,
        )

    def back(wave, step):
        return pltpu.make_async_remote_copy(
            src_ref=finished.at[wave, step],
            dst_ref=returned.at[wave, step],
            send_sem=back_send.at[wave, step],
            recv_sem=back_recv.at[wave, step],
            device_id={AXIS: behind(step)},
            device_id_type=pl.DeviceIdType.MESH,
        )

    loads = [
        pltpu.make_async_copy(tokens_hbm, tokens, load_sem.at[0]),
        pltpu.make_async_copy(gate_hbm, gate, load_sem.at[1]),
        pltpu.make_async_copy(up_hbm, up, load_sem.at[2]),
        pltpu.make_async_copy(down_hbm, down, load_sem.at[3]),
    ]
    for load in loads:
        load.start()

    barrier = pltpu.get_barrier_semaphore()

    def greet(step, carry):
        pl.semaphore_signal(
            barrier, inc=1, device_id={AXIS: ahead(step)}, device_id_type=pl.DeviceIdType.MESH
        )
        return carry

    lax.fori_loop(1, devices, greet, 0)

    expert = lax.broadcasted_iota(jnp.int32, (LANES, tok_rows), 0)
    named = jnp.zeros((LANES, tok_rows), jnp.float32)
    share = jnp.zeros((LANES, tok_rows), jnp.float32)
    for k in range(fanout):
        hit = expert == ids_ref[k : k + 1, :]
        named = jnp.where(hit, 1.0, named)
        share = jnp.where(hit, weights_ref[k : k + 1, :], share)
    before = (
        lax.broadcasted_iota(jnp.int32, (tok_rows, tok_rows), 0)
        < lax.broadcasted_iota(jnp.int32, (tok_rows, tok_rows), 1)
    )
    count = jnp.dot(
        named.astype(jnp.bfloat16),
        jnp.where(before, 1.0, 0.0).astype(jnp.bfloat16),
        preferred_element_type=jnp.float32,
    )
    place = jnp.where(named > 0.5, count, -1.0)
    place_rows[...] = place
    place_cols[...] = place.T
    share_cols[...] = share.T
    image = jnp.broadcast_to(modality_ref[...].astype(jnp.float32), (LANES, tok_rows)).T

    loads[0].wait()
    rows = 64
    for start in range(0, tok_rows, rows):
        values = tokens[start : start + rows, :].astype(jnp.float32)
        square = jnp.mean(values * values, axis=1, keepdims=True)
        gains = jnp.where(
            image[start : start + rows, :1] > 0.5, gain_ref[1:2, :], gain_ref[0:1, :]
        )
        normed[start : start + rows, :] = (
            values * lax.rsqrt(square + epsilon) * gains
        ).astype(jnp.bfloat16)

    def pack(wave, step, target):
        line = place_rows[pl.ds(ahead(step), 1), :]
        slot = lax.broadcasted_iota(jnp.int32, (chunk, tok_rows), 0) + wave * chunk
        pick = jnp.where(line == slot.astype(jnp.float32), 1.0, 0.0).astype(jnp.bfloat16)
        target[wave, step] = jnp.dot(
            pick, normed[...], preferred_element_type=jnp.float32
        ).astype(jnp.bfloat16)

    others = devices - 1
    items = waves * others

    def which(item):
        return item // others, others - item % others

    pl.semaphore_wait(barrier, others)

    def send(item, carry):
        wave, step = which(item)
        pack(wave, step, packed)
        go(wave, step).start()
        return carry

    lax.fori_loop(0, items, send, 0)

    for load in loads[1:]:
        load.wait()

    def feed(source, target, wave, step):
        value = source[wave, step]
        opened = jnp.dot(value, gate[...], preferred_element_type=jnp.float32)
        upper = jnp.dot(value, up[...], preferred_element_type=jnp.float32)
        active = (opened / (1.0 + jnp.exp(-opened)) * upper).astype(jnp.bfloat16)
        target[wave, step] = jnp.dot(
            active, down[...], preferred_element_type=jnp.float32
        ).astype(jnp.bfloat16)

    def spread(wave, step):
        lane = lax.broadcasted_iota(jnp.int32, (tok_rows, LANES), 1) == ahead(step)
        line = jnp.sum(jnp.where(lane, place_cols[...], 0.0), axis=1, keepdims=True)
        worth = jnp.sum(jnp.where(lane, share_cols[...], 0.0), axis=1, keepdims=True)
        slot = lax.broadcasted_iota(jnp.int32, (tok_rows, chunk), 1) + wave * chunk
        spots = jnp.where(line == slot.astype(jnp.float32), worth, 0.0)
        high = spots.astype(jnp.bfloat16)
        low = (spots - high.astype(jnp.float32)).astype(jnp.bfloat16)
        value = returned[wave, step]
        return jnp.dot(high, value, preferred_element_type=jnp.float32) + jnp.dot(
            low, value, preferred_element_type=jnp.float32
        )

    total[...] = tokens[...].astype(jnp.float32)

    def local(wave, carry):
        pack(wave, 0, arrived)
        feed(arrived, returned, wave, 0)
        total[...] += spread(wave, 0)
        return carry

    lax.fori_loop(0, waves, local, 0)

    def serve(item, carry):
        wave, step = which(item)
        go(wave, step).wait_recv()
        feed(arrived, finished, wave, step)
        back(wave, step).start()
        return carry

    lax.fori_loop(0, items, serve, 0)

    def collect(item, carry):
        wave, step = which(item)
        back(wave, step).wait_recv()
        total[...] += spread(wave, step)
        return carry

    lax.fori_loop(0, items - 1, collect, 0)
    wave, step = which(items - 1)
    back(wave, step).wait_recv()
    out_ref[...] = (total[...] + spread(wave, step)).astype(out_ref.dtype)

    def settle(item, carry):
        wave, step = which(item)
        go(wave, step).wait_send()
        back(wave, step).wait_send()
        return carry

    lax.fori_loop(0, items, settle, 0)


def pair_kernel(
    blocks,
    groups,
    pieces,
    tokens_hbm,
    modality_hbm,
    ids_hbm,
    weights_hbm,
    gain_hbm,
    gate_hbm,
    up_hbm,
    down_hbm,
    out_ref,
    modality_ref,
    ids_ref,
    weights_ref,
    gain_ref,
    tokens,
    sorted_tokens,
    near_tokens,
    gate,
    up,
    down,
    far_gate,
    far_up,
    far_down,
    normed,
    near_normed,
    total,
    near_total,
    facts,
    sorted_facts,
    near_facts,
    slots,
    columns,
    active,
    sum_out,
    sum_in,
    load_sem,
    facts_sem,
    dense_send,
    dense_recv,
    sum_send,
    sum_recv,
    wide_send,
    wide_recv,
    tall_send,
    tall_recv,
):
    tok_rows, width = tokens.shape
    hidden = gate.shape[1]
    fanout = ids_ref.shape[0]
    devices = lax.axis_size(AXIS)
    capacity = tok_rows * fanout * 5 // (4 * devices)
    part = tok_rows // blocks
    free = (tok_rows - capacity) // part
    me = lax.axis_index(AXIS)
    copy_of = lax.axis_index("dp")
    layer, core = copy_of // 2, copy_of % 2
    beside = me // 2 * 2 + 1 - me % 2
    above = (1 - me // 2) * 2 + me % 2
    diagonal = (1 - me // 2) * 2 + 1 - me % 2
    other_layer = (layer // 2 * 2 + 1 - layer % 2) * 2 + core
    other_core = layer * 2 + 1 - core
    quarter = layer % 2 * 2 + core
    layer_quarter = (1 - layer % 2) * 2 + core

    def remote(source, target, send_sem, recv_sem, copy, peer):
        return pltpu.make_async_remote_copy(
            src_ref=source,
            dst_ref=target,
            send_sem=send_sem,
            recv_sem=recv_sem,
            device_id={"dp": copy, AXIS: peer},
            device_id_type=pl.DeviceIdType.MESH,
        )

    def part_rows(block):
        return pl.ds(pl.multiple_of(block * part, part), part)

    def dense(block):
        rows = part_rows(block)
        return remote(
            sorted_tokens.at[rows],
            near_tokens.at[rows],
            dense_send.at[block],
            dense_recv.at[block],
            copy_of,
            beside,
        )

    def sums(block):
        rows = part_rows(block)
        return remote(
            sum_out.at[rows],
            sum_in.at[rows],
            sum_send.at[0, block],
            sum_recv.at[0, block],
            copy_of,
            beside,
        )

    half = width // 2
    halves = (pl.ds(0, half), pl.ds(half, half))

    def late_sums(side, block):
        rows = part_rows(block)
        return remote(
            sum_out.at[rows, halves[side]],
            sum_in.at[rows, halves[side]],
            sum_send.at[side, block],
            sum_recv.at[side, block],
            copy_of,
            beside,
        )

    wide_rows = width // 4 // groups
    tall_rows = hidden // 4 // pieces

    def weight_copy(stage, kind, index):
        which = layer_quarter if stage == 3 else quarter
        if kind < 2:
            near, far = ((gate_hbm, far_gate), (up_hbm, far_up))[kind]
            send, recv = wide_send.at[kind], wide_recv.at[kind]
            start = which * (width // 4) + index * wide_rows
            spot = (pl.ds(pl.multiple_of(start, wide_rows), wide_rows),)
        else:
            near, far, send, recv = down_hbm, far_down, tall_send, tall_recv
            start = which * (hidden // 4) + index % pieces * tall_rows
            spot = (pl.ds(pl.multiple_of(start, tall_rows), tall_rows), halves[index // pieces])
        copy, peer = ((copy_of, above), (other_layer, me), (other_core, me), (other_core, me))[stage]
        return remote(
            (near if stage == 0 else far).at[spot],
            far.at[spot],
            send.at[stage, index],
            recv.at[stage, index],
            copy,
            peer,
        )

    def arrived_across(kind, index):
        weight_copy(0, kind, index).wait_recv()
        weight_copy(1, kind, index).start()
        weight_copy(2, kind, index).start()

    def arrived_along(kind, index):
        weight_copy(1, kind, index).wait_recv()
        weight_copy(3, kind, index).start()

    def each(count, step, start=0):
        def body(index, carry):
            step(index)
            return carry

        lax.fori_loop(start, count, body, 0)

    loads = [
        pltpu.make_async_copy(source, target, load_sem.at[index])
        for index, (source, target) in enumerate(
            (
                (ids_hbm, ids_ref),
                (weights_hbm, weights_ref),
                (modality_hbm, modality_ref),
                (tokens_hbm, tokens),
                (gain_hbm, gain_ref),
                (gate_hbm, gate),
                (up_hbm, up),
                (down_hbm, down),
            )
        )
    ]
    for load in loads[:5]:
        load.start()
    barrier = pltpu.get_barrier_semaphore()
    for copy, peer in ((copy_of, beside), (copy_of, above), (other_layer, me), (other_core, me)):
        pl.semaphore_signal(
            barrier,
            inc=1,
            device_id={"dp": copy, AXIS: peer},
            device_id_type=pl.DeviceIdType.MESH,
        )
    for load in loads[:3]:
        load.wait()

    lines = 8
    expert = lax.broadcasted_iota(jnp.int32, (lines, tok_rows), 0)
    named = jnp.zeros((lines, tok_rows), jnp.float32)
    share = jnp.where(
        expert == devices,
        jnp.broadcast_to(modality_ref[...].astype(jnp.float32), (lines, tok_rows)),
        0.0,
    )
    late = jnp.zeros((1, tok_rows), jnp.float32)
    for k in range(fanout):
        share = jnp.where(expert == ids_ref[k : k + 1, :], weights_ref[k : k + 1, :], share)
        late = jnp.where(ids_ref[k : k + 1, :] == diagonal, 1.0, late)
    facts[...] = share
    named = jnp.where(expert == 0, late, 1.0 - late)
    before = (
        lax.broadcasted_iota(jnp.int32, (tok_rows, tok_rows), 0)
        < lax.broadcasted_iota(jnp.int32, (tok_rows, tok_rows), 1)
    )
    count = jnp.dot(
        named.astype(jnp.bfloat16),
        jnp.where(before, 1.0, 0.0).astype(jnp.bfloat16),
        preferred_element_type=jnp.float32,
    )
    slots[...] = jnp.broadcast_to(
        jnp.where(late > 0.5, tok_rows - 1.0 - count[0:1, :], count[1:2, :]), (lines, tok_rows)
    )

    def sort(block):
        slot = lax.broadcasted_iota(jnp.int32, (part, tok_rows), 0) + block * part
        pick = jnp.where(slots[0:1, :] == slot.astype(jnp.float32), 1.0, 0.0).astype(jnp.bfloat16)
        sorted_tokens[part_rows(block)] = jnp.dot(
            pick, tokens[...], preferred_element_type=jnp.float32
        ).astype(jnp.bfloat16)

    loads[3].wait()
    for load in loads[5:]:
        load.start()
    sort(0)
    pl.semaphore_wait(barrier, 4)
    dense(0).start()
    each(groups, lambda index: [weight_copy(0, kind, index).start() for kind in range(2)])
    for index in range(2 * pieces):
        weight_copy(0, 2, index).start()

    def keep(place, line):
        columns[place] = jnp.broadcast_to(line, (LANES, tok_rows)).T

    own_mine, own_far, near_mine, near_far, near_image, own_image, own_slot = range(7)
    keep(own_slot, slots[0:1, :])
    keep(own_mine, facts[pl.ds(me, 1), :])
    keep(own_far, facts[pl.ds(above, 1), :])
    keep(own_image, facts[devices : devices + 1, :])

    def places(start, count):
        slot = lax.broadcasted_iota(jnp.int32, (tok_rows, count), 1) + start
        here = columns[own_slot, :, 0:1] == slot.astype(jnp.float32)
        return jnp.where(here, 1.0, 0.0).astype(jnp.bfloat16)

    coarse = share.astype(jnp.bfloat16)
    fine = (share - coarse.astype(jnp.float32)).astype(jnp.bfloat16)
    every = places(0, tok_rows)
    sorted_facts[...] = jnp.dot(coarse, every, preferred_element_type=jnp.float32) + jnp.dot(
        fine, every, preferred_element_type=jnp.float32
    )
    told = remote(sorted_facts, near_facts, facts_sem.at[0], facts_sem.at[1], copy_of, beside)
    told.start()

    def leave(block):
        sort(block)
        dense(block).start()

    each(blocks, leave, 1)

    def normalize(source, target, image, rows):
        values = source[rows, :].astype(jnp.float32)
        square = jnp.mean(values * values, axis=1, keepdims=True)
        gains = jnp.where(image > 0.5, gain_ref[1:2, :], gain_ref[0:1, :])
        target[rows, :] = (values * lax.rsqrt(square + epsilon) * gains).astype(jnp.bfloat16)

    def activate(value, opening, upping):
        opened = jnp.dot(value, opening[...], preferred_element_type=jnp.float32)
        upper = jnp.dot(value, upping[...], preferred_element_type=jnp.float32)
        return (opened / (1.0 + jnp.exp(-opened)) * upper).astype(jnp.bfloat16)

    def settle(value, closing):
        result = jnp.dot(value, closing, preferred_element_type=jnp.float32)
        return result.astype(jnp.bfloat16).astype(jnp.float32)

    def feed(value, opening, upping, closing):
        return settle(activate(value, opening, upping), closing[...])

    loads[4].wait()
    rows = 64

    def ready(index):
        here = pl.ds(pl.multiple_of(index * rows, rows), rows)
        normalize(tokens, normed, columns[own_image, here, 0:1], here)

    each(tok_rows // rows, ready)
    for load in loads[5:]:
        load.wait()

    batch = tok_rows // groups

    def batch_rows(group):
        return pl.ds(pl.multiple_of(group * batch, batch), batch)

    double = 2 * batch

    def pair_rows(group):
        return pl.ds(pl.multiple_of(group * double, double), double)

    def both(group):
        arrived_across(0, group)

        @pl.when(group < tok_rows // double)
        def _():
            here = pair_rows(group)
            total[here, :] = tokens[here, :].astype(jnp.float32) + columns[
                own_mine, here, 0:1
            ] * feed(normed[here, :], gate, up, down)

        @pl.when(group > 0)
        def _():
            arrived_along(1, group - 1)

        arrived_across(1, group)

        @pl.when(group == 0)
        def _():
            told.wait_recv()
            keep(near_mine, near_facts[pl.ds(me, 1), :])
            keep(near_far, near_facts[pl.ds(above, 1), :])
            keep(near_image, near_facts[devices : devices + 1, :])

        @pl.when(group == groups - 1)
        def _():
            arrived_across(2, 0)

        for index in range(blocks // groups):
            dense(group * (blocks // groups) + index).wait_recv()
        here = batch_rows(group)
        for start in range(0, batch, rows):
            few = pl.ds(pl.multiple_of(group * batch + start, rows), rows)
            normalize(near_tokens, near_normed, columns[near_image, few, 0:1], few)
        near = columns[near_mine, here, 0:1] * feed(near_normed[here, :], gate, up, down)
        near_total[here, :] = near
        sum_out[here, :] = near.astype(jnp.bfloat16)
        for index in range(blocks // groups):
            block = group * (blocks // groups) + index

            @pl.when(block < free)
            def _():
                sums(block).start()

        arrived_along(0, group)

    each(groups, both)
    arrived_along(1, groups - 1)
    arrived_across(2, 1)

    def joined(kind, index):
        weight_copy(2, kind, index).wait_recv()
        weight_copy(3, kind, index).wait_recv()

    late = slice(free * part, tok_rows)
    each(groups, lambda index: [joined(kind, index) for kind in range(2)])
    active[...] = activate(near_normed[late, :], far_gate, far_up)

    def finish(side):
        for index in range(side * pieces, (side + 1) * pieces):
            joined(2, index)
        there = slice(side * half, (side + 1) * half)
        sum_out[late, there] = (
            near_total[late, there]
            + columns[near_far, late, 0:1] * settle(active[...], far_down[:, there])
        ).astype(jnp.bfloat16)
        each(blocks, lambda block: late_sums(side, block).start(), free)

    arrived_along(2, 0)
    arrived_across(2, 2)
    arrived_along(2, 1)
    finish(0)
    arrived_across(2, 3)
    arrived_along(2, 2)
    each(free, lambda block: sums(block).wait_recv())
    total[...] += jnp.dot(
        places(0, free * part), sum_in[: free * part, :], preferred_element_type=jnp.float32
    )
    arrived_along(2, 3)
    finish(1)

    def own(group):
        here = pair_rows(group)
        total[here, :] += columns[own_far, here, 0:1] * feed(
            normed[here, :], far_gate, far_up, far_down
        )

    each(tok_rows // double, own)

    def take(side, first, last):
        each(last, lambda block: late_sums(side, block).wait_recv(), first)
        there = slice(side * half, (side + 1) * half)
        some = slice(first * part, last * part)
        out_ref[:, there] = (
            total[:, there]
            + jnp.dot(
                places(first * part, (last - first) * part),
                sum_in[some, there],
                preferred_element_type=jnp.float32,
            )
        ).astype(out_ref.dtype)

    take(0, free, blocks)
    each(blocks - 1, lambda block: late_sums(1, block).wait_recv(), free)
    total[:, half:] += jnp.dot(
        places(free * part, (blocks - 1 - free) * part),
        sum_in[free * part : (blocks - 1) * part, half:],
        preferred_element_type=jnp.float32,
    )
    take(1, blocks - 1, blocks)

    told.wait_send()
    each(blocks, lambda block: dense(block).wait_send())
    each(free, lambda block: sums(block).wait_send())
    for side in range(2):
        each(blocks, lambda block: late_sums(side, block).wait_send(), free)

    def sent(kind, index):
        for stage in range(4):
            weight_copy(stage, kind, index).wait_send()

    each(groups, lambda index: [sent(kind, index) for kind in range(2)])
    for index in range(2 * pieces):
        sent(2, index)


def pair_scratch(tok_rows, width, hidden, fanout, capacity, blocks, groups, pieces):
    dense = pltpu.VMEM((tok_rows, width), jnp.bfloat16)
    sums = pltpu.VMEM((tok_rows, width), jnp.float32)
    facts = pltpu.VMEM((8, tok_rows), jnp.float32)
    wide = pltpu.VMEM((width, hidden), jnp.bfloat16)
    tall = pltpu.VMEM((hidden, width), jnp.bfloat16)
    by_block = pltpu.SemaphoreType.DMA((blocks,))
    by_group = pltpu.SemaphoreType.DMA((2, 4, groups))
    by_piece = pltpu.SemaphoreType.DMA((4, 2 * pieces))
    by_side = pltpu.SemaphoreType.DMA((2, blocks))
    part = tok_rows // blocks
    late = tok_rows - (tok_rows - capacity) // part * part
    return [
        pltpu.VMEM((1, tok_rows), jnp.int32), pltpu.VMEM((fanout, tok_rows), jnp.int32),
        pltpu.VMEM((fanout, tok_rows), jnp.float32), pltpu.VMEM((2, width), jnp.float32),
        dense, dense, dense, wide, wide, tall, wide, wide, tall, dense, dense, sums, sums,
        facts, facts, facts, facts, pltpu.VMEM((7, tok_rows, LANES), jnp.float32),
        pltpu.VMEM((late, hidden), jnp.bfloat16), dense, dense,
        pltpu.SemaphoreType.DMA((8,)), pltpu.SemaphoreType.DMA((2,)),
        by_block, by_block, by_side, by_side, by_group, by_group, by_piece, by_piece,
    ]


def direct_scratch(tok_rows, width, hidden, buffer, sems):
    return [
        pltpu.VMEM((tok_rows, width), jnp.bfloat16),
        pltpu.VMEM((width, hidden), jnp.bfloat16),
        pltpu.VMEM((width, hidden), jnp.bfloat16),
        pltpu.VMEM((hidden, width), jnp.bfloat16),
        pltpu.VMEM((tok_rows, width), jnp.bfloat16),
        pltpu.VMEM((tok_rows, width), jnp.float32),
        pltpu.VMEM((LANES, tok_rows), jnp.float32),
        pltpu.VMEM((tok_rows, LANES), jnp.float32),
        pltpu.VMEM((tok_rows, LANES), jnp.float32),
        buffer,
        buffer,
        buffer,
        buffer,
        pltpu.SemaphoreType.DMA((4,)),
        sems,
        sems,
        sems,
        sems,
    ]


def shards(
    tokens, modality, expert_ids, route_weights, norm_gain, gate_weight, up_weight, down_weight
):
    devices = lax.axis_size(AXIS)
    tok_rows, width = tokens.shape
    fanout = expert_ids.shape[1]
    hidden = gate_weight.shape[1]
    capacity = min(tok_rows, tok_rows * fanout * 5 // (4 * devices))
    waves = 2 if capacity % 32 == 0 and capacity >= 256 else 1
    chunk = capacity // waves
    buffer = pltpu.VMEM((waves, devices, chunk, width), jnp.bfloat16)
    near = pl.BlockSpec(memory_space=pltpu.VMEM)
    far = pl.BlockSpec(memory_space=pl.ANY)
    sems = pltpu.SemaphoreType.DMA((waves, devices))
    blocks, groups, pieces = 8, 4, 2
    paired = (
        devices == 4
        and lax.axis_size("dp") % 4 == 0
        and tok_rows % (LANES * groups) == 0
        and tok_rows % (64 * blocks) == 0
        and width % (64 * groups) == 0
        and hidden % 128 == 0
    )
    if paired:
        kernel = functools.partial(pair_kernel, blocks, groups, pieces)
        scratch = pair_scratch(tok_rows, width, hidden, fanout, capacity, blocks, groups, pieces)
    else:
        kernel = functools.partial(moe_kernel, devices)
        scratch = direct_scratch(tok_rows, width, hidden, buffer, sems)
    return pl.pallas_call(
        kernel,
        out_shape=pltpu.VMEM((tok_rows, width), jnp.bfloat16),
        in_specs=[far] + [far if paired else near] * 4 + [far] * 3,
        out_specs=near,
        scratch_shapes=scratch,
        compiler_params=pltpu.CompilerParams(
            collective_id=0, has_side_effects=True, vmem_limit_bytes=(60 if paired else 58) * 1024 * 1024
        ),
    )(
        tokens,
        modality.reshape(1, tok_rows),
        expert_ids.T,
        route_weights.T,
        norm_gain,
        gate_weight,
        up_weight,
        down_weight,
    )


def solution(mesh):
    placed = (
        P(("dp", AXIS), None),
        P(("dp", AXIS)),
        P(("dp", AXIS), None),
        P(("dp", AXIS), None),
        P(),
        P(None, AXIS),
        P(None, AXIS),
        P(AXIS, None),
    )
    return jax.shard_map(
        shards, mesh=mesh, in_specs=placed, out_specs=P(("dp", AXIS), None), check_vma=False
    )
```

```python
import functools

import jax
import jax.numpy as jnp
from jax import lax
from jax.experimental import pallas as pl
from jax.experimental.pallas import tpu as pltpu
from jax.sharding import PartitionSpec as P

epsilon = 1e-05
LANES = 128
AXIS = "expert"


def grid_side(devices):
    side = 1
    while side * side < devices:
        side += 1
    return side if side * side == devices else devices


def moe_kernel(
    devices,
    tokens_hbm,
    modality_ref,
    ids_ref,
    weights_ref,
    gain_ref,
    gate_hbm,
    up_hbm,
    down_hbm,
    out_ref,
    tokens,
    gate,
    up,
    down,
    normed,
    total,
    place_rows,
    place_cols,
    share_cols,
    packed,
    arrived,
    finished,
    returned,
    load_sem,
    go_send,
    go_recv,
    back_send,
    back_recv,
):
    waves, _, chunk, width = packed.shape
    tok_rows = tokens.shape[0]
    fanout = ids_ref.shape[0]
    me = lax.axis_index(AXIS)
    side = grid_side(devices)
    mine_hi, mine_lo = me // side, me % side
    lines = devices // side

    def ahead(step):
        return ((mine_hi + step // side) % lines) * side + (mine_lo + step % side) % side

    def behind(step):
        return ((mine_hi + lines - step // side) % lines) * side + (
            mine_lo + side - step % side
        ) % side

    def go(wave, step):
        return pltpu.make_async_remote_copy(
            src_ref=packed.at[wave, step],
            dst_ref=arrived.at[wave, step],
            send_sem=go_send.at[wave, step],
            recv_sem=go_recv.at[wave, step],
            device_id={AXIS: ahead(step)},
            device_id_type=pl.DeviceIdType.MESH,
        )

    def back(wave, step):
        return pltpu.make_async_remote_copy(
            src_ref=finished.at[wave, step],
            dst_ref=returned.at[wave, step],
            send_sem=back_send.at[wave, step],
            recv_sem=back_recv.at[wave, step],
            device_id={AXIS: behind(step)},
            device_id_type=pl.DeviceIdType.MESH,
        )

    loads = [
        pltpu.make_async_copy(tokens_hbm, tokens, load_sem.at[0]),
        pltpu.make_async_copy(gate_hbm, gate, load_sem.at[1]),
        pltpu.make_async_copy(up_hbm, up, load_sem.at[2]),
        pltpu.make_async_copy(down_hbm, down, load_sem.at[3]),
    ]
    for load in loads:
        load.start()

    barrier = pltpu.get_barrier_semaphore()

    def greet(step, carry):
        pl.semaphore_signal(
            barrier, inc=1, device_id={AXIS: ahead(step)}, device_id_type=pl.DeviceIdType.MESH
        )
        return carry

    lax.fori_loop(1, devices, greet, 0)

    expert = lax.broadcasted_iota(jnp.int32, (LANES, tok_rows), 0)
    named = jnp.zeros((LANES, tok_rows), jnp.float32)
    share = jnp.zeros((LANES, tok_rows), jnp.float32)
    for k in range(fanout):
        hit = expert == ids_ref[k : k + 1, :]
        named = jnp.where(hit, 1.0, named)
        share = jnp.where(hit, weights_ref[k : k + 1, :], share)
    before = (
        lax.broadcasted_iota(jnp.int32, (tok_rows, tok_rows), 0)
        < lax.broadcasted_iota(jnp.int32, (tok_rows, tok_rows), 1)
    )
    count = jnp.dot(
        named.astype(jnp.bfloat16),
        jnp.where(before, 1.0, 0.0).astype(jnp.bfloat16),
        preferred_element_type=jnp.float32,
    )
    place = jnp.where(named > 0.5, count, -1.0)
    place_rows[...] = place
    place_cols[...] = place.T
    share_cols[...] = share.T
    image = jnp.broadcast_to(modality_ref[...].astype(jnp.float32), (LANES, tok_rows)).T

    loads[0].wait()
    rows = 64
    for start in range(0, tok_rows, rows):
        values = tokens[start : start + rows, :].astype(jnp.float32)
        square = jnp.mean(values * values, axis=1, keepdims=True)
        gains = jnp.where(
            image[start : start + rows, :1] > 0.5, gain_ref[1:2, :], gain_ref[0:1, :]
        )
        normed[start : start + rows, :] = (
            values * lax.rsqrt(square + epsilon) * gains
        ).astype(jnp.bfloat16)

    def pack(wave, step, target):
        line = place_rows[pl.ds(ahead(step), 1), :]
        slot = lax.broadcasted_iota(jnp.int32, (chunk, tok_rows), 0) + wave * chunk
        pick = jnp.where(line == slot.astype(jnp.float32), 1.0, 0.0).astype(jnp.bfloat16)
        target[wave, step] = jnp.dot(
            pick, normed[...], preferred_element_type=jnp.float32
        ).astype(jnp.bfloat16)

    others = devices - 1
    items = waves * others

    def which(item):
        return item // others, others - item % others

    pl.semaphore_wait(barrier, others)

    def send(item, carry):
        wave, step = which(item)
        pack(wave, step, packed)
        go(wave, step).start()
        return carry

    lax.fori_loop(0, items, send, 0)

    for load in loads[1:]:
        load.wait()

    def feed(source, target, wave, step):
        value = source[wave, step]
        opened = jnp.dot(value, gate[...], preferred_element_type=jnp.float32)
        upper = jnp.dot(value, up[...], preferred_element_type=jnp.float32)
        active = (opened / (1.0 + jnp.exp(-opened)) * upper).astype(jnp.bfloat16)
        target[wave, step] = jnp.dot(
            active, down[...], preferred_element_type=jnp.float32
        ).astype(jnp.bfloat16)

    def spread(wave, step):
        lane = lax.broadcasted_iota(jnp.int32, (tok_rows, LANES), 1) == ahead(step)
        line = jnp.sum(jnp.where(lane, place_cols[...], 0.0), axis=1, keepdims=True)
        worth = jnp.sum(jnp.where(lane, share_cols[...], 0.0), axis=1, keepdims=True)
        slot = lax.broadcasted_iota(jnp.int32, (tok_rows, chunk), 1) + wave * chunk
        spots = jnp.where(line == slot.astype(jnp.float32), worth, 0.0)
        high = spots.astype(jnp.bfloat16)
        low = (spots - high.astype(jnp.float32)).astype(jnp.bfloat16)
        value = returned[wave, step]
        return jnp.dot(high, value, preferred_element_type=jnp.float32) + jnp.dot(
            low, value, preferred_element_type=jnp.float32
        )

    total[...] = tokens[...].astype(jnp.float32)

    def local(wave, carry):
        pack(wave, 0, arrived)
        feed(arrived, returned, wave, 0)
        total[...] += spread(wave, 0)
        return carry

    lax.fori_loop(0, waves, local, 0)

    def serve(item, carry):
        wave, step = which(item)
        go(wave, step).wait_recv()
        feed(arrived, finished, wave, step)
        back(wave, step).start()
        return carry

    lax.fori_loop(0, items, serve, 0)

    def collect(item, carry):
        wave, step = which(item)
        back(wave, step).wait_recv()
        total[...] += spread(wave, step)
        return carry

    lax.fori_loop(0, items - 1, collect, 0)
    wave, step = which(items - 1)
    back(wave, step).wait_recv()
    out_ref[...] = (total[...] + spread(wave, step)).astype(out_ref.dtype)

    def settle(item, carry):
        wave, step = which(item)
        go(wave, step).wait_send()
        back(wave, step).wait_send()
        return carry

    lax.fori_loop(0, items, settle, 0)


def pair_kernel(
    blocks,
    groups,
    sides,
    tokens_hbm,
    modality_hbm,
    ids_hbm,
    weights_hbm,
    gain_hbm,
    gate_hbm,
    up_hbm,
    down_hbm,
    out_ref,
    modality_ref,
    ids_ref,
    weights_ref,
    gain_ref,
    tokens,
    sorted_tokens,
    near_tokens,
    gate,
    up,
    down,
    far_gate,
    far_up,
    far_down,
    normed,
    near_normed,
    total,
    near_total,
    facts,
    sorted_facts,
    near_facts,
    slots,
    columns,
    active,
    own_active,
    relayed,
    sum_out,
    sum_in,
    load_sem,
    facts_sem,
    dense_send,
    dense_recv,
    sum_send,
    sum_recv,
    wide_send,
    wide_recv,
    tall_send,
    tall_recv,
    out_send,
    out_recv,
    home_send,
    home_recv,
):
    tok_rows, width = tokens.shape
    hidden = gate.shape[1]
    fanout = ids_ref.shape[0]
    devices = lax.axis_size(AXIS)
    capacity = tok_rows * fanout * 5 // (4 * devices)
    part = tok_rows // blocks
    free = (tok_rows - capacity) // part
    me = lax.axis_index(AXIS)
    copy_of = lax.axis_index("dp")
    layer, core = copy_of // 2, copy_of % 2
    beside = me // 2 * 2 + 1 - me % 2
    above = (1 - me // 2) * 2 + me % 2
    kind_of = layer // 2 % 2
    first = beside * (1 - kind_of) + above * kind_of
    second = above * (1 - kind_of) + beside * kind_of
    diagonal = (1 - me // 2) * 2 + 1 - me % 2
    other_layer = (layer // 2 * 2 + 1 - layer % 2) * 2 + core
    other_core = layer * 2 + 1 - core
    far_layer = (layer // 4 * 4 + (layer + 2) % 4) * 2 + core
    quarter = layer % 2 * 2 + core
    layer_quarter = (1 - layer % 2) * 2 + core

    def remote(source, target, send_sem, recv_sem, copy, peer):
        return pltpu.make_async_remote_copy(
            src_ref=source,
            dst_ref=target,
            send_sem=send_sem,
            recv_sem=recv_sem,
            device_id={"dp": copy, AXIS: peer},
            device_id_type=pl.DeviceIdType.MESH,
        )

    def part_rows(block):
        return pl.ds(pl.multiple_of(block * part, part), part)

    def dense(block):
        rows = part_rows(block)
        return remote(
            sorted_tokens.at[rows],
            near_tokens.at[rows],
            dense_send.at[block],
            dense_recv.at[block],
            copy_of,
            first,
        )

    def sums(block):
        rows = part_rows(block)
        return remote(
            sum_out.at[rows],
            sum_in.at[rows],
            sum_send.at[0, block],
            sum_recv.at[0, block],
            copy_of,
            first,
        )

    slim = width // sides

    def columns_of(side):
        return pl.ds(side * slim, slim)

    def late_sums(side, block):
        rows = part_rows(block)
        return remote(
            sum_out.at[rows, columns_of(side)],
            sum_in.at[rows, columns_of(side)],
            sum_send.at[side, block],
            sum_recv.at[side, block],
            copy_of,
            first,
        )

    detours = blocks - free - 1

    def out(index):
        rows = part_rows(index)
        return remote(
            sum_out.at[part_rows(free + index), columns_of(0)],
            relayed.at[rows],
            out_send.at[index],
            out_recv.at[index],
            far_layer,
            first,
        )

    def home(index):
        rows = part_rows(index)
        return remote(
            relayed.at[rows],
            sum_in.at[part_rows(free + index), columns_of(0)],
            home_send.at[index],
            home_recv.at[index],
            far_layer,
            me,
        )

    wide_rows = width // 4 // groups
    tall_rows = hidden // 4

    def weight_copy(stage, kind, index):
        which = layer_quarter if stage in (3, 4) else quarter
        if kind < 2:
            near, far = ((gate_hbm, far_gate), (up_hbm, far_up))[kind]
            send, recv = wide_send.at[kind], wide_recv.at[kind]
            start = which * (width // 4) + index * wide_rows
            spot = (pl.ds(pl.multiple_of(start, wide_rows), wide_rows),)
        else:
            near, far, send, recv = down_hbm, far_down, tall_send, tall_recv
            start = which * tall_rows
            spot = (pl.ds(pl.multiple_of(start, tall_rows), tall_rows), columns_of(index))
        copy, peer = (
            (copy_of, second),
            (other_layer, me),
            (other_core, me),
            (other_core, me),
            (copy_of, second),
        )[stage]
        return remote(
            (near if stage in (0, 4) else far).at[spot],
            far.at[spot],
            send.at[stage, index],
            recv.at[stage, index],
            copy,
            peer,
        )

    def arrived_across(kind, index):
        weight_copy(0, kind, index).wait_recv()
        if kind < 2 or index < sides - 1:
            weight_copy(1, kind, index).start()
        weight_copy(2, kind, index).start()

    def arrived_along(kind, index):
        weight_copy(1 if kind < 2 or index < sides - 1 else 4, kind, index).wait_recv()
        weight_copy(3, kind, index).start()

    def each(count, step, start=0):
        def body(index, carry):
            step(index)
            return carry

        lax.fori_loop(start, count, body, 0)

    loads = [
        pltpu.make_async_copy(source, target, load_sem.at[index])
        for index, (source, target) in enumerate(
            (
                (ids_hbm, ids_ref),
                (weights_hbm, weights_ref),
                (modality_hbm, modality_ref),
                (tokens_hbm, tokens),
                (gain_hbm, gain_ref),
                (gate_hbm, gate),
                (up_hbm, up),
                (down_hbm, down),
            )
        )
    ]
    barrier = pltpu.get_barrier_semaphore()
    partners = (
        (far_layer, first),
        (far_layer, second),
        (far_layer, me),
        (copy_of, first),
        (copy_of, second),
        (other_layer, me),
        (other_core, me),
    )
    for copy, peer in partners:
        pl.semaphore_signal(
            barrier,
            inc=1,
            device_id={"dp": copy, AXIS: peer},
            device_id_type=pl.DeviceIdType.MESH,
        )
    for load in loads[:5]:
        load.start()
    for load in loads[:3]:
        load.wait()

    lines = 8
    expert = lax.broadcasted_iota(jnp.int32, (lines, tok_rows), 0)
    named = jnp.zeros((lines, tok_rows), jnp.float32)
    share = jnp.where(
        expert == devices,
        jnp.broadcast_to(modality_ref[...].astype(jnp.float32), (lines, tok_rows)),
        0.0,
    )
    late = jnp.zeros((1, tok_rows), jnp.float32)
    for k in range(fanout):
        share = jnp.where(expert == ids_ref[k : k + 1, :], weights_ref[k : k + 1, :], share)
        late = jnp.where(ids_ref[k : k + 1, :] == diagonal, 1.0, late)
    facts[...] = share
    named = jnp.where(expert == 0, late, 1.0 - late)
    before = (
        lax.broadcasted_iota(jnp.int32, (tok_rows, tok_rows), 0)
        < lax.broadcasted_iota(jnp.int32, (tok_rows, tok_rows), 1)
    )
    count = jnp.dot(
        named.astype(jnp.bfloat16),
        jnp.where(before, 1.0, 0.0).astype(jnp.bfloat16),
        preferred_element_type=jnp.float32,
    )
    slots[...] = jnp.broadcast_to(
        jnp.where(late > 0.5, tok_rows - 1.0 - count[0:1, :], count[1:2, :]), (lines, tok_rows)
    )

    def sort(block):
        slot = lax.broadcasted_iota(jnp.int32, (part, tok_rows), 0) + block * part
        pick = jnp.where(slots[0:1, :] == slot.astype(jnp.float32), 1.0, 0.0).astype(jnp.bfloat16)
        sorted_tokens[part_rows(block)] = jnp.dot(
            pick, tokens[...], preferred_element_type=jnp.float32
        ).astype(jnp.bfloat16)

    loads[3].wait()
    for load in loads[5:]:
        load.start()
    sort(0)
    pl.semaphore_wait(barrier, len(partners))
    dense(0).start()
    each(groups, lambda index: [weight_copy(0, kind, index).start() for kind in range(2)])
    for side in range(sides):
        weight_copy(0, 2, side).start()
    weight_copy(4, 2, sides - 1).start()

    def keep(place, line):
        columns[place] = jnp.broadcast_to(line, (LANES, tok_rows)).T

    own_mine, own_far, near_mine, near_far, near_image, own_image, own_slot = range(7)
    keep(own_slot, slots[0:1, :])
    keep(own_mine, facts[pl.ds(me, 1), :])
    keep(own_far, facts[pl.ds(second, 1), :])
    keep(own_image, facts[devices : devices + 1, :])

    def places(start, count):
        slot = lax.broadcasted_iota(jnp.int32, (tok_rows, count), 1) + start
        here = columns[own_slot, :, 0:1] == slot.astype(jnp.float32)
        return jnp.where(here, 1.0, 0.0).astype(jnp.bfloat16)

    coarse = share.astype(jnp.bfloat16)
    fine = (share - coarse.astype(jnp.float32)).astype(jnp.bfloat16)
    every = places(0, tok_rows)
    sorted_facts[...] = jnp.dot(coarse, every, preferred_element_type=jnp.float32) + jnp.dot(
        fine, every, preferred_element_type=jnp.float32
    )
    told = remote(sorted_facts, near_facts, facts_sem.at[0], facts_sem.at[1], copy_of, first)
    told.start()

    def leave(block):
        sort(block)
        dense(block).start()

    each(blocks, leave, 1)

    def normalize(source, target, image, rows):
        values = source[rows, :].astype(jnp.float32)
        square = jnp.mean(values * values, axis=1, keepdims=True)
        gains = jnp.where(image > 0.5, gain_ref[1:2, :], gain_ref[0:1, :])
        target[rows, :] = (values * lax.rsqrt(square + epsilon) * gains).astype(jnp.bfloat16)

    def activate(value, opening, upping):
        opened = jnp.dot(value, opening[...], preferred_element_type=jnp.float32)
        upper = jnp.dot(value, upping[...], preferred_element_type=jnp.float32)
        return (opened / (1.0 + jnp.exp(-opened)) * upper).astype(jnp.bfloat16)

    def settle(value, closing):
        result = jnp.dot(value, closing, preferred_element_type=jnp.float32)
        return result.astype(jnp.bfloat16).astype(jnp.float32)

    def feed(value, opening, upping, closing):
        return settle(activate(value, opening, upping), closing[...])

    loads[4].wait()
    rows = 64

    def ready(index):
        here = pl.ds(pl.multiple_of(index * rows, rows), rows)
        normalize(tokens, normed, columns[own_image, here, 0:1], here)

    each(tok_rows // rows, ready)
    for load in loads[5:]:
        load.wait()

    batch = tok_rows // groups

    def batch_rows(group):
        return pl.ds(pl.multiple_of(group * batch, batch), batch)

    double = 2 * batch

    def pair_rows(group):
        return pl.ds(pl.multiple_of(group * double, double), double)

    def both(group):
        arrived_across(0, group)

        @pl.when(group < tok_rows // double)
        def _():
            here = pair_rows(group)
            total[here, :] = tokens[here, :].astype(jnp.float32) + columns[
                own_mine, here, 0:1
            ] * feed(normed[here, :], gate, up, down)

        @pl.when(group > 0)
        def _():
            arrived_along(1, group - 1)

        arrived_across(1, group)

        @pl.when(group == 0)
        def _():
            told.wait_recv()
            keep(near_mine, near_facts[pl.ds(me, 1), :])
            keep(near_far, near_facts[pl.ds(second, 1), :])
            keep(near_image, near_facts[devices : devices + 1, :])

        @pl.when(group == groups - 1)
        def _():
            arrived_across(2, 0)

        for index in range(blocks // groups):
            dense(group * (blocks // groups) + index).wait_recv()
        here = batch_rows(group)
        for start in range(0, batch, rows):
            few = pl.ds(pl.multiple_of(group * batch + start, rows), rows)
            normalize(near_tokens, near_normed, columns[near_image, few, 0:1], few)
        near = columns[near_mine, here, 0:1] * feed(near_normed[here, :], gate, up, down)
        near_total[here, :] = near
        sum_out[here, :] = near.astype(jnp.bfloat16)
        for index in range(blocks // groups):
            block = group * (blocks // groups) + index

            @pl.when(block < free)
            def _():
                sums(block).start()

        arrived_along(0, group)

    each(groups, both)
    arrived_along(1, groups - 1)
    arrived_across(2, 1)

    def joined(kind, index):
        weight_copy(2, kind, index).wait_recv()
        weight_copy(3, kind, index).wait_recv()

    late = slice(free * part, tok_rows)
    each(groups, lambda index: [joined(kind, index) for kind in range(2)])
    active[...] = activate(near_normed[late, :], far_gate, far_up)

    def finish(side):
        joined(2, side)
        there = slice(side * slim, (side + 1) * slim)
        sum_out[late, there] = (
            near_total[late, there]
            + columns[near_far, late, 0:1] * settle(active[...], far_down[:, there])
        ).astype(jnp.bfloat16)
        if side == 0:
            each(detours, lambda index: out(index).start())
        each(blocks, lambda block: late_sums(side, block).start(), direct(side))

    def direct(side):
        return free + detours if side == 0 else free

    def pass_on(index):
        out(index).wait_recv()
        home(index).start()

    def own(group):
        here = pair_rows(group)
        own_active[here, :] = activate(normed[here, :], far_gate, far_up)

    def own_finish(side):
        there = slice(side * slim, (side + 1) * slim)
        total[:, there] += columns[own_far, :, 0:1] * settle(own_active[...], far_down[:, there])

    arrived_along(2, 0)
    finish(0)
    arrived_across(2, 2)
    arrived_along(2, 1)
    finish(1)
    own(0)
    arrived_across(2, 3)
    arrived_along(2, 2)
    finish(2)
    each(detours // 2, pass_on)
    each(tok_rows // double, own, 1)
    arrived_along(2, 3)
    finish(3)
    each(detours, pass_on, detours // 2)
    each(free, lambda block: sums(block).wait_recv())
    total[...] += jnp.dot(
        places(0, free * part), sum_in[: free * part, :], preferred_element_type=jnp.float32
    )
    for side in range(sides):
        own_finish(side)

    def gathered(side, begin, end):
        return total[:, side * slim : (side + 1) * slim] + jnp.dot(
            places(begin * part, (end - begin) * part),
            sum_in[begin * part : end * part, side * slim : (side + 1) * slim],
            preferred_element_type=jnp.float32,
        )

    def take(side):
        out_ref[:, side * slim : (side + 1) * slim] = gathered(side, free, blocks).astype(
            out_ref.dtype
        )

    for side in range(1, sides - 1):
        each(blocks, lambda block: late_sums(side, block).wait_recv(), free)
        take(side)
    each(detours, lambda index: home(index).wait_recv())
    each(blocks, lambda block: late_sums(0, block).wait_recv(), direct(0))
    take(0)
    side = sides - 1
    there = slice(side * slim, width)
    each(blocks - 1, lambda block: late_sums(side, block).wait_recv(), free)
    total[:, there] = gathered(side, free, blocks - 1)
    late_sums(side, blocks - 1).wait_recv()
    out_ref[:, there] = gathered(side, blocks - 1, blocks).astype(out_ref.dtype)

    told.wait_send()
    each(blocks, lambda block: dense(block).wait_send())
    each(free, lambda block: sums(block).wait_send())
    for side in range(sides):
        each(blocks, lambda block: late_sums(side, block).wait_send(), direct(side))
    each(detours, lambda index: out(index).wait_send())
    each(detours, lambda index: home(index).wait_send())

    def sent(kind, index):
        straight = kind == 2 and index == sides - 1
        for stage in (0, 4, 2, 3) if straight else range(4):
            weight_copy(stage, kind, index).wait_send()

    each(groups, lambda index: [sent(kind, index) for kind in range(2)])
    for side in range(sides):
        sent(2, side)


def pair_scratch(tok_rows, width, hidden, fanout, capacity, blocks, groups, sides):
    dense = pltpu.VMEM((tok_rows, width), jnp.bfloat16)
    sums = pltpu.VMEM((tok_rows, width), jnp.float32)
    facts = pltpu.VMEM((8, tok_rows), jnp.float32)
    wide = pltpu.VMEM((width, hidden), jnp.bfloat16)
    tall = pltpu.VMEM((hidden, width), jnp.bfloat16)
    by_block = pltpu.SemaphoreType.DMA((blocks,))
    by_group = pltpu.SemaphoreType.DMA((2, 4, groups))
    by_piece = pltpu.SemaphoreType.DMA((5, sides))
    by_side = pltpu.SemaphoreType.DMA((sides, blocks))
    part = tok_rows // blocks
    late = tok_rows - (tok_rows - capacity) // part * part
    return [
        pltpu.VMEM((1, tok_rows), jnp.int32), pltpu.VMEM((fanout, tok_rows), jnp.int32),
        pltpu.VMEM((fanout, tok_rows), jnp.float32), pltpu.VMEM((2, width), jnp.float32),
        dense, dense, dense, wide, wide, tall, wide, wide, tall, dense, dense, sums, sums,
        facts, facts, facts, facts, pltpu.VMEM((7, tok_rows, LANES), jnp.float32),
        pltpu.VMEM((late, hidden), jnp.bfloat16), pltpu.VMEM((tok_rows, hidden), jnp.bfloat16),
        pltpu.VMEM((late, width // sides), jnp.bfloat16), dense, dense,
        pltpu.SemaphoreType.DMA((8,)), pltpu.SemaphoreType.DMA((2,)),
        by_block, by_block, by_side, by_side, by_group, by_group, by_piece, by_piece,
        by_block, by_block, by_block, by_block,
    ]


def direct_scratch(tok_rows, width, hidden, buffer, sems):
    return [
        pltpu.VMEM((tok_rows, width), jnp.bfloat16),
        pltpu.VMEM((width, hidden), jnp.bfloat16),
        pltpu.VMEM((width, hidden), jnp.bfloat16),
        pltpu.VMEM((hidden, width), jnp.bfloat16),
        pltpu.VMEM((tok_rows, width), jnp.bfloat16),
        pltpu.VMEM((tok_rows, width), jnp.float32),
        pltpu.VMEM((LANES, tok_rows), jnp.float32),
        pltpu.VMEM((tok_rows, LANES), jnp.float32),
        pltpu.VMEM((tok_rows, LANES), jnp.float32),
        buffer,
        buffer,
        buffer,
        buffer,
        pltpu.SemaphoreType.DMA((4,)),
        sems,
        sems,
        sems,
        sems,
    ]


def shards(
    tokens, modality, expert_ids, route_weights, norm_gain, gate_weight, up_weight, down_weight
):
    devices = lax.axis_size(AXIS)
    tok_rows, width = tokens.shape
    fanout = expert_ids.shape[1]
    hidden = gate_weight.shape[1]
    capacity = min(tok_rows, tok_rows * fanout * 5 // (4 * devices))
    waves = 2 if capacity % 32 == 0 and capacity >= 256 else 1
    chunk = capacity // waves
    buffer = pltpu.VMEM((waves, devices, chunk, width), jnp.bfloat16)
    near = pl.BlockSpec(memory_space=pltpu.VMEM)
    far = pl.BlockSpec(memory_space=pl.ANY)
    sems = pltpu.SemaphoreType.DMA((waves, devices))
    blocks, groups, sides = 8, 4, 4
    paired = (
        devices == 4
        and lax.axis_size("dp") % 8 == 0
        and tok_rows % (LANES * groups) == 0
        and tok_rows % (64 * blocks) == 0
        and width % (64 * groups) == 0
        and width % (LANES * sides) == 0
        and hidden % 128 == 0
    )
    if paired:
        kernel = functools.partial(pair_kernel, blocks, groups, sides)
        scratch = pair_scratch(tok_rows, width, hidden, fanout, capacity, blocks, groups, sides)
    else:
        kernel = functools.partial(moe_kernel, devices)
        scratch = direct_scratch(tok_rows, width, hidden, buffer, sems)
    return pl.pallas_call(
        kernel,
        out_shape=pltpu.VMEM((tok_rows, width), jnp.bfloat16),
        in_specs=[far] + [far if paired else near] * 4 + [far] * 3,
        out_specs=near,
        scratch_shapes=scratch,
        compiler_params=pltpu.CompilerParams(
            collective_id=0, has_side_effects=True, vmem_limit_bytes=(60 if paired else 58) * 1024 * 1024
        ),
    )(
        tokens,
        modality.reshape(1, tok_rows),
        expert_ids.T,
        route_weights.T,
        norm_gain,
        gate_weight,
        up_weight,
        down_weight,
    )


def solution(mesh):
    placed = (
        P(("dp", AXIS), None),
        P(("dp", AXIS)),
        P(("dp", AXIS), None),
        P(("dp", AXIS), None),
        P(),
        P(None, AXIS),
        P(None, AXIS),
        P(AXIS, None),
    )
    return jax.shard_map(
        shards, mesh=mesh, in_specs=placed, out_specs=P(("dp", AXIS), None), check_vma=False
    )
```

```python
import functools

import jax
import jax.numpy as jnp
from jax import lax
from jax.experimental import pallas as pl
from jax.experimental.pallas import tpu as pltpu
from jax.sharding import PartitionSpec as P

epsilon = 1e-05
LANES = 128
AXIS = "expert"


def grid_side(devices):
    side = 1
    while side * side < devices:
        side += 1
    return side if side * side == devices else devices


def moe_kernel(
    devices,
    tokens_hbm,
    modality_ref,
    ids_ref,
    weights_ref,
    gain_ref,
    gate_hbm,
    up_hbm,
    down_hbm,
    out_ref,
    tokens,
    gate,
    up,
    down,
    normed,
    total,
    place_rows,
    place_cols,
    share_cols,
    packed,
    arrived,
    finished,
    returned,
    load_sem,
    go_send,
    go_recv,
    back_send,
    back_recv,
):
    waves, _, chunk, width = packed.shape
    tok_rows = tokens.shape[0]
    fanout = ids_ref.shape[0]
    me = lax.axis_index(AXIS)
    side = grid_side(devices)
    mine_hi, mine_lo = me // side, me % side
    lines = devices // side

    def ahead(step):
        return ((mine_hi + step // side) % lines) * side + (mine_lo + step % side) % side

    def behind(step):
        return ((mine_hi + lines - step // side) % lines) * side + (
            mine_lo + side - step % side
        ) % side

    def go(wave, step):
        return pltpu.make_async_remote_copy(
            src_ref=packed.at[wave, step],
            dst_ref=arrived.at[wave, step],
            send_sem=go_send.at[wave, step],
            recv_sem=go_recv.at[wave, step],
            device_id={AXIS: ahead(step)},
            device_id_type=pl.DeviceIdType.MESH,
        )

    def back(wave, step):
        return pltpu.make_async_remote_copy(
            src_ref=finished.at[wave, step],
            dst_ref=returned.at[wave, step],
            send_sem=back_send.at[wave, step],
            recv_sem=back_recv.at[wave, step],
            device_id={AXIS: behind(step)},
            device_id_type=pl.DeviceIdType.MESH,
        )

    loads = [
        pltpu.make_async_copy(tokens_hbm, tokens, load_sem.at[0]),
        pltpu.make_async_copy(gate_hbm, gate, load_sem.at[1]),
        pltpu.make_async_copy(up_hbm, up, load_sem.at[2]),
        pltpu.make_async_copy(down_hbm, down, load_sem.at[3]),
    ]
    for load in loads:
        load.start()

    barrier = pltpu.get_barrier_semaphore()

    def greet(step, carry):
        pl.semaphore_signal(
            barrier, inc=1, device_id={AXIS: ahead(step)}, device_id_type=pl.DeviceIdType.MESH
        )
        return carry

    lax.fori_loop(1, devices, greet, 0)

    expert = lax.broadcasted_iota(jnp.int32, (LANES, tok_rows), 0)
    named = jnp.zeros((LANES, tok_rows), jnp.float32)
    share = jnp.zeros((LANES, tok_rows), jnp.float32)
    for k in range(fanout):
        hit = expert == ids_ref[k : k + 1, :]
        named = jnp.where(hit, 1.0, named)
        share = jnp.where(hit, weights_ref[k : k + 1, :], share)
    before = (
        lax.broadcasted_iota(jnp.int32, (tok_rows, tok_rows), 0)
        < lax.broadcasted_iota(jnp.int32, (tok_rows, tok_rows), 1)
    )
    count = jnp.dot(
        named.astype(jnp.bfloat16),
        jnp.where(before, 1.0, 0.0).astype(jnp.bfloat16),
        preferred_element_type=jnp.float32,
    )
    place = jnp.where(named > 0.5, count, -1.0)
    place_rows[...] = place
    place_cols[...] = place.T
    share_cols[...] = share.T
    image = jnp.broadcast_to(modality_ref[...].astype(jnp.float32), (LANES, tok_rows)).T

    loads[0].wait()
    rows = 64
    for start in range(0, tok_rows, rows):
        values = tokens[start : start + rows, :].astype(jnp.float32)
        square = jnp.mean(values * values, axis=1, keepdims=True)
        gains = jnp.where(
            image[start : start + rows, :1] > 0.5, gain_ref[1:2, :], gain_ref[0:1, :]
        )
        normed[start : start + rows, :] = (
            values * lax.rsqrt(square + epsilon) * gains
        ).astype(jnp.bfloat16)

    def pack(wave, step, target):
        line = place_rows[pl.ds(ahead(step), 1), :]
        slot = lax.broadcasted_iota(jnp.int32, (chunk, tok_rows), 0) + wave * chunk
        pick = jnp.where(line == slot.astype(jnp.float32), 1.0, 0.0).astype(jnp.bfloat16)
        target[wave, step] = jnp.dot(
            pick, normed[...], preferred_element_type=jnp.float32
        ).astype(jnp.bfloat16)

    others = devices - 1
    items = waves * others

    def which(item):
        return item // others, others - item % others

    pl.semaphore_wait(barrier, others)

    def send(item, carry):
        wave, step = which(item)
        pack(wave, step, packed)
        go(wave, step).start()
        return carry

    lax.fori_loop(0, items, send, 0)

    for load in loads[1:]:
        load.wait()

    def feed(source, target, wave, step):
        value = source[wave, step]
        opened = jnp.dot(value, gate[...], preferred_element_type=jnp.float32)
        upper = jnp.dot(value, up[...], preferred_element_type=jnp.float32)
        active = (opened / (1.0 + jnp.exp(-opened)) * upper).astype(jnp.bfloat16)
        target[wave, step] = jnp.dot(
            active, down[...], preferred_element_type=jnp.float32
        ).astype(jnp.bfloat16)

    def spread(wave, step):
        lane = lax.broadcasted_iota(jnp.int32, (tok_rows, LANES), 1) == ahead(step)
        line = jnp.sum(jnp.where(lane, place_cols[...], 0.0), axis=1, keepdims=True)
        worth = jnp.sum(jnp.where(lane, share_cols[...], 0.0), axis=1, keepdims=True)
        slot = lax.broadcasted_iota(jnp.int32, (tok_rows, chunk), 1) + wave * chunk
        spots = jnp.where(line == slot.astype(jnp.float32), worth, 0.0)
        high = spots.astype(jnp.bfloat16)
        low = (spots - high.astype(jnp.float32)).astype(jnp.bfloat16)
        value = returned[wave, step]
        return jnp.dot(high, value, preferred_element_type=jnp.float32) + jnp.dot(
            low, value, preferred_element_type=jnp.float32
        )

    total[...] = tokens[...].astype(jnp.float32)

    def local(wave, carry):
        pack(wave, 0, arrived)
        feed(arrived, returned, wave, 0)
        total[...] += spread(wave, 0)
        return carry

    lax.fori_loop(0, waves, local, 0)

    def serve(item, carry):
        wave, step = which(item)
        go(wave, step).wait_recv()
        feed(arrived, finished, wave, step)
        back(wave, step).start()
        return carry

    lax.fori_loop(0, items, serve, 0)

    def collect(item, carry):
        wave, step = which(item)
        back(wave, step).wait_recv()
        total[...] += spread(wave, step)
        return carry

    lax.fori_loop(0, items - 1, collect, 0)
    wave, step = which(items - 1)
    back(wave, step).wait_recv()
    out_ref[...] = (total[...] + spread(wave, step)).astype(out_ref.dtype)

    def settle(item, carry):
        wave, step = which(item)
        go(wave, step).wait_send()
        back(wave, step).wait_send()
        return carry

    lax.fori_loop(0, items, settle, 0)


def pair_kernel(
    blocks,
    groups,
    sides,
    tokens_hbm,
    modality_hbm,
    ids_hbm,
    weights_hbm,
    gain_hbm,
    gate_hbm,
    up_hbm,
    down_hbm,
    out_ref,
    modality_ref,
    ids_ref,
    weights_ref,
    gain_ref,
    tokens,
    sorted_tokens,
    near_tokens,
    gate,
    up,
    down,
    far_gate,
    far_up,
    far_down,
    normed,
    near_normed,
    total,
    near_total,
    facts,
    sorted_facts,
    near_facts,
    slots,
    columns,
    active,
    own_active,
    relayed,
    sum_out,
    sum_in,
    load_sem,
    facts_sem,
    dense_send,
    dense_recv,
    sum_send,
    sum_recv,
    late_send,
    late_recv,
    wide_send,
    wide_recv,
    wide_join,
    tall_send,
    tall_recv,
    tall_join,
    out_send,
    out_recv,
    home_send,
    home_recv,
    entered,
):
    tok_rows, width = tokens.shape
    hidden = gate.shape[1]
    fanout = ids_ref.shape[0]
    devices = lax.axis_size(AXIS)
    capacity = tok_rows * fanout * 5 // (4 * devices)
    part = tok_rows // blocks
    free = (tok_rows - capacity) // part
    me = lax.axis_index(AXIS)
    copy_of = lax.axis_index("dp")
    layer, core = copy_of // 2, copy_of % 2
    beside = me // 2 * 2 + 1 - me % 2
    above = (1 - me // 2) * 2 + me % 2
    kind_of = layer // 2 % 2
    first = beside * (1 - kind_of) + above * kind_of
    second = above * (1 - kind_of) + beside * kind_of
    diagonal = (1 - me // 2) * 2 + 1 - me % 2
    other_layer = (layer // 2 * 2 + 1 - layer % 2) * 2 + core
    other_core = layer * 2 + 1 - core
    beside_layers = 1 + (layer % 4 + 1) // 2 % 2
    middle = beside_layers == 2
    across_layer = (layer // 4 * 4 + 3 - layer % 4) * 2 + core
    far_layer = (layer // 4 * 4 + (layer + 2) % 4) * 2 + core
    quarter = layer % 2 * 2 + core
    layer_quarter = (1 - layer % 2) * 2 + core

    def remote(source, target, send_sem, recv_sem, copy, peer):
        return pltpu.make_async_remote_copy(
            src_ref=source,
            dst_ref=target,
            send_sem=send_sem,
            recv_sem=recv_sem,
            device_id={"dp": copy, AXIS: peer},
            device_id_type=pl.DeviceIdType.MESH,
        )

    def part_rows(block):
        return pl.ds(pl.multiple_of(block * part, part), part)

    share_of = blocks // groups
    batch = tok_rows // groups

    def batch_rows(group):
        return pl.ds(pl.multiple_of(group * batch, batch), batch)

    def dense_rows(rows, group):
        return remote(
            sorted_tokens.at[rows],
            near_tokens.at[rows],
            dense_send,
            dense_recv.at[group],
            copy_of,
            first,
        )

    def dense(block):
        return dense_rows(part_rows(block), block // share_of)

    def sums_rows(rows):
        return remote(sum_out.at[rows], sum_in.at[rows], sum_send, sum_recv, copy_of, first)

    def sums(block):
        return sums_rows(part_rows(block))

    slim = width // sides

    def columns_of(side):
        return pl.ds(side * slim, slim)

    detours = blocks - free - 1

    def late_rows(index):
        begin = {0: free + detours, sides: blocks - 1}.get(index, free)
        end = blocks - 1 if index == sides - 1 else blocks
        return pl.ds(begin * part, (end - begin) * part)

    def late_sums(index):
        spot = (late_rows(index), columns_of(min(index, sides - 1)))
        return remote(
            sum_out.at[spot],
            sum_in.at[spot],
            late_send.at[index],
            late_recv.at[index],
            copy_of,
            first,
        )

    def out_rows(begin, end, which):
        rows = pl.ds(begin * part, (end - begin) * part)
        return remote(
            sum_out.at[pl.ds((free + begin) * part, (end - begin) * part), columns_of(0)],
            relayed.at[rows],
            out_send,
            out_recv.at[which],
            far_layer,
            first,
        )

    def home_rows(begin, end):
        return remote(
            relayed.at[pl.ds(begin * part, (end - begin) * part)],
            sum_in.at[pl.ds((free + begin) * part, (end - begin) * part), columns_of(0)],
            home_send,
            home_recv,
            far_layer,
            me,
        )

    cut = detours // 2
    spans = ((0, cut), (cut, detours))

    wide_rows = width // 4 // groups
    tall_rows = hidden // 4

    def weight_copy(stage, kind, index):
        which = layer_quarter if stage in (3, 4) else quarter
        if kind < 2:
            near, far = ((gate_hbm, far_gate), (up_hbm, far_up))[kind]
            send = wide_send.at[stage]
            recv = wide_join if stage in (2, 3) else wide_recv.at[kind, stage, index]
            start = which * (width // 4) + index * wide_rows
            spot = (pl.ds(pl.multiple_of(start, wide_rows), wide_rows),)
        else:
            near, far, send = down_hbm, far_down, tall_send.at[stage]
            recv = tall_join.at[index] if stage in (2, 3) else tall_recv.at[stage % 3, index]
            start = which * tall_rows
            spot = (pl.ds(pl.multiple_of(start, tall_rows), tall_rows), columns_of(index))
        return weight_remote(
            stage, (near if stage in (0, 4) else far).at[spot], far.at[spot], send, recv
        )

    def weight_remote(stage, source, target, send, recv):
        copy, peer = (
            (copy_of, second),
            (other_layer, me),
            (other_core, me),
            (other_core, me),
            (copy_of, second),
        )[stage]
        return remote(source, target, send, recv, copy, peer)

    def wide_joined():
        weight_remote(2, far_gate, far_gate, wide_send.at[2], wide_join).wait_recv()

    def tall_joined(side):
        both = far_down.at[pl.ds(0, 2 * tall_rows), columns_of(side)]
        weight_remote(2, both, both, tall_send.at[2], tall_join.at[side]).wait_recv()

    def weights_sent():
        wide = far_gate.at[pl.ds(0, width // 2)]
        for stage in range(4):
            weight_remote(stage, wide, wide, wide_send.at[stage], wide_join).wait_send()
        for stage, wholes in enumerate((sides, sides - 1, sides, sides, 1)):
            tall = far_down.at[pl.ds(0, tall_rows), pl.ds(0, wholes * slim)]
            weight_remote(stage, tall, tall, tall_send.at[stage], tall_join.at[0]).wait_send()

    def arrived_across(kind, index):
        weight_copy(0, kind, index).wait_recv()
        if kind < 2 or index < sides - 1:
            weight_copy(1, kind, index).start()
        weight_copy(2, kind, index).start()

    def arrived_along(kind, index):
        weight_copy(1 if kind < 2 or index < sides - 1 else 4, kind, index).wait_recv()
        weight_copy(3, kind, index).start()

    def each(count, step, start=0):
        def body(index, carry):
            step(index)
            return carry

        lax.fori_loop(start, count, body, 0)

    loads = [
        pltpu.make_async_copy(source, target, load_sem.at[index])
        for index, (source, target) in enumerate(
            (
                (ids_hbm, ids_ref),
                (weights_hbm, weights_ref),
                (modality_hbm, modality_ref),
                (tokens_hbm, tokens),
                (gain_hbm, gain_ref),
                (gate_hbm, gate),
                (up_hbm, up),
                (down_hbm, down),
            )
        )
    ]
    barrier = pltpu.get_barrier_semaphore()
    partners = (
        (copy_of, first),
        (copy_of, second),
        (other_layer, me),
        (other_core, me),
    )

    def tell(semaphore, copy, peer):
        pl.semaphore_signal(
            semaphore,
            inc=1,
            device_id={"dp": copy, AXIS: peer},
            device_id_type=pl.DeviceIdType.MESH,
        )

    def along_line(step):
        step(other_layer)

        @pl.when(middle)
        def _():
            step(across_layer)

    for copy, peer in partners:
        tell(barrier, copy, peer)

    @pl.when(middle)
    def _():
        tell(barrier, across_layer, me)

    for load in loads[:5]:
        load.start()
    for load in loads[:3]:
        load.wait()

    lines = 8
    expert = lax.broadcasted_iota(jnp.int32, (lines, tok_rows), 0)
    named = jnp.zeros((lines, tok_rows), jnp.float32)
    share = jnp.where(
        expert == devices,
        jnp.broadcast_to(modality_ref[...].astype(jnp.float32), (lines, tok_rows)),
        0.0,
    )
    late = jnp.zeros((1, tok_rows), jnp.float32)
    for k in range(fanout):
        share = jnp.where(expert == ids_ref[k : k + 1, :], weights_ref[k : k + 1, :], share)
        late = jnp.where(ids_ref[k : k + 1, :] == diagonal, 1.0, late)
    facts[...] = share
    named = jnp.where(expert == 0, late, 1.0 - late)
    before = (
        lax.broadcasted_iota(jnp.int32, (tok_rows, tok_rows), 0)
        < lax.broadcasted_iota(jnp.int32, (tok_rows, tok_rows), 1)
    )
    count = jnp.dot(
        named.astype(jnp.bfloat16),
        jnp.where(before, 1.0, 0.0).astype(jnp.bfloat16),
        preferred_element_type=jnp.float32,
    )
    slots[...] = jnp.broadcast_to(
        jnp.where(late > 0.5, tok_rows - 1.0 - count[0:1, :], count[1:2, :]), (lines, tok_rows)
    )

    def sort(block):
        slot = lax.broadcasted_iota(jnp.int32, (part, tok_rows), 0) + block * part
        pick = jnp.where(slots[0:1, :] == slot.astype(jnp.float32), 1.0, 0.0).astype(jnp.bfloat16)
        sorted_tokens[part_rows(block)] = jnp.dot(
            pick, tokens[...], preferred_element_type=jnp.float32
        ).astype(jnp.bfloat16)

    loads[3].wait()
    for load in loads[5:]:
        load.start()
    sort(0)
    sort(1)
    pl.semaphore_wait(barrier, len(partners) - 1 + beside_layers)

    dense(0).start()
    dense(1).start()
    along_line(lambda copy: tell(entered.at[0], copy, me))
    each(groups, lambda index: [weight_copy(0, kind, index).start() for kind in range(2)])
    for side in range(sides):
        weight_copy(0, 2, side).start()
    weight_copy(4, 2, sides - 1).start()

    def keep(place, line):
        columns[place] = jnp.broadcast_to(line, (LANES, tok_rows)).T

    own_mine, own_far, near_mine, near_far, near_image, own_image, own_slot = range(7)
    keep(own_slot, slots[0:1, :])
    keep(own_mine, facts[pl.ds(me, 1), :])
    keep(own_far, facts[pl.ds(second, 1), :])
    keep(own_image, facts[devices : devices + 1, :])

    def places(start, count):
        slot = lax.broadcasted_iota(jnp.int32, (tok_rows, count), 1) + start
        here = columns[own_slot, :, 0:1] == slot.astype(jnp.float32)
        return jnp.where(here, 1.0, 0.0).astype(jnp.bfloat16)

    coarse = share.astype(jnp.bfloat16)
    fine = (share - coarse.astype(jnp.float32)).astype(jnp.bfloat16)
    every = places(0, tok_rows)
    sorted_facts[...] = jnp.dot(coarse, every, preferred_element_type=jnp.float32) + jnp.dot(
        fine, every, preferred_element_type=jnp.float32
    )
    told = remote(sorted_facts, near_facts, facts_sem.at[0], facts_sem.at[1], copy_of, first)
    told.start()

    def leave(block):
        sort(block)
        dense(block).start()

    each(blocks, leave, 2)

    def normalize(source, target, image, rows):
        values = source[rows, :].astype(jnp.float32)
        square = jnp.mean(values * values, axis=1, keepdims=True)
        gains = jnp.where(image > 0.5, gain_ref[1:2, :], gain_ref[0:1, :])
        target[rows, :] = (values * lax.rsqrt(square + epsilon) * gains).astype(jnp.bfloat16)

    def activate(value, opening, upping):
        opened = jnp.dot(value, opening[...], preferred_element_type=jnp.float32)
        upper = jnp.dot(value, upping[...], preferred_element_type=jnp.float32)
        return (opened / (1.0 + jnp.exp(-opened)) * upper).astype(jnp.bfloat16)

    def settle(value, closing):
        result = jnp.dot(value, closing, preferred_element_type=jnp.float32)
        return result.astype(jnp.bfloat16).astype(jnp.float32)

    def feed(value, opening, upping, closing):
        return settle(activate(value, opening, upping), closing[...])

    loads[4].wait()
    rows = 64

    def ready(index):
        here = pl.ds(pl.multiple_of(index * rows, rows), rows)
        normalize(tokens, normed, columns[own_image, here, 0:1], here)

    each(tok_rows // rows, ready)
    pl.semaphore_wait(entered.at[0], beside_layers)
    along_line(lambda copy: tell(entered.at[1], copy, me))
    for load in loads[5:]:
        load.wait()

    double = 2 * batch

    def pair_rows(group):
        return pl.ds(pl.multiple_of(group * double, double), double)

    def both(group):
        arrived_across(0, group)

        @pl.when(group < tok_rows // double)
        def _():
            here = pair_rows(group)
            total[here, :] = tokens[here, :].astype(jnp.float32) + columns[
                own_mine, here, 0:1
            ] * feed(normed[here, :], gate, up, down)

        @pl.when(group > 0)
        def _():
            arrived_along(1, group - 1)

        arrived_across(1, group)

        @pl.when(group == 0)
        def _():
            told.wait_recv()
            keep(near_mine, near_facts[pl.ds(me, 1), :])
            keep(near_far, near_facts[pl.ds(second, 1), :])
            keep(near_image, near_facts[devices : devices + 1, :])

        @pl.when(group == groups - 1)
        def _():
            arrived_across(2, 0)

        here = batch_rows(group)
        dense_rows(here, group).wait_recv()
        for start in range(0, batch, rows):
            few = pl.ds(pl.multiple_of(group * batch + start, rows), rows)
            normalize(near_tokens, near_normed, columns[near_image, few, 0:1], few)
        near = columns[near_mine, here, 0:1] * feed(near_normed[here, :], gate, up, down)
        near_total[here, :] = near
        sum_out[here, :] = near.astype(jnp.bfloat16)
        for index in range(share_of):
            block = group * share_of + index

            @pl.when(block < free)
            def _():
                sums(block).start()

        arrived_along(0, group)

    each(groups, both)
    arrived_along(1, groups - 1)
    arrived_across(2, 1)

    late = slice(free * part, tok_rows)
    wide_joined()
    active[...] = activate(near_normed[late, :], far_gate, far_up)

    def finish(side):
        tall_joined(side)
        there = slice(side * slim, (side + 1) * slim)
        sum_out[late, there] = (
            near_total[late, there]
            + columns[near_far, late, 0:1] * settle(active[...], far_down[:, there])
        ).astype(jnp.bfloat16)
        if side == 0:
            for which, (begin, end) in enumerate(spans):
                out_rows(begin, end, which).start()
        late_sums(side).start()
        if side == sides - 1:
            late_sums(sides).start()

    def pass_on(which):
        begin, end = spans[which]
        out_rows(begin, end, which).wait_recv()
        home_rows(begin, end).start()

    def own(group):
        here = pair_rows(group)
        own_active[here, :] = activate(normed[here, :], far_gate, far_up)

    def own_finish(side):
        there = slice(side * slim, (side + 1) * slim)
        total[:, there] += columns[own_far, :, 0:1] * settle(own_active[...], far_down[:, there])

    pl.semaphore_wait(entered.at[1], beside_layers)
    arrived_along(2, 0)
    finish(0)
    arrived_across(2, 2)
    arrived_along(2, 1)
    finish(1)
    own(0)
    arrived_across(2, 3)
    arrived_along(2, 2)
    finish(2)
    pass_on(0)
    each(tok_rows // double, own, 1)
    arrived_along(2, 3)
    finish(3)
    pass_on(1)
    sums_rows(pl.ds(0, free * part)).wait_recv()
    total[...] += jnp.dot(
        places(0, free * part), sum_in[: free * part, :], preferred_element_type=jnp.float32
    )
    for side in range(sides):
        own_finish(side)

    def gathered(side, begin, end):
        return total[:, side * slim : (side + 1) * slim] + jnp.dot(
            places(begin * part, (end - begin) * part),
            sum_in[begin * part : end * part, side * slim : (side + 1) * slim],
            preferred_element_type=jnp.float32,
        )

    def take(side):
        out_ref[:, side * slim : (side + 1) * slim] = gathered(side, free, blocks).astype(
            out_ref.dtype
        )

    for side in range(1, sides - 1):
        late_sums(side).wait_recv()
        take(side)
    home_rows(0, detours).wait_recv()
    late_sums(0).wait_recv()
    take(0)
    told.wait_send()
    dense_rows(pl.ds(0, tok_rows), 0).wait_send()
    sums_rows(pl.ds(0, free * part)).wait_send()
    for side in range(sides - 1):
        late_sums(side).wait_send()
    out_rows(0, detours, 0).wait_send()
    home_rows(0, detours).wait_send()
    weights_sent()

    side = sides - 1
    there = slice(side * slim, width)
    late_sums(side).wait_recv()
    total[:, there] = gathered(side, free, blocks - 1)
    late_sums(sides).wait_recv()
    out_ref[:, there] = gathered(side, blocks - 1, blocks).astype(out_ref.dtype)
    late_sums(side).wait_send()
    late_sums(sides).wait_send()


def pair_scratch(tok_rows, width, hidden, fanout, capacity, blocks, groups, sides):
    dense = pltpu.VMEM((tok_rows, width), jnp.bfloat16)
    sums = pltpu.VMEM((tok_rows, width), jnp.float32)
    facts = pltpu.VMEM((8, tok_rows), jnp.float32)
    wide = pltpu.VMEM((width, hidden), jnp.bfloat16)
    tall = pltpu.VMEM((hidden, width), jnp.bfloat16)
    semaphores = pltpu.SemaphoreType.DMA
    one = semaphores(())
    part = tok_rows // blocks
    late = tok_rows - (tok_rows - capacity) // part * part
    return [
        pltpu.VMEM((1, tok_rows), jnp.int32), pltpu.VMEM((fanout, tok_rows), jnp.int32),
        pltpu.VMEM((fanout, tok_rows), jnp.float32), pltpu.VMEM((2, width), jnp.float32),
        dense, dense, dense, wide, wide, tall, wide, wide, tall, dense, dense, sums, sums,
        facts, facts, facts, facts, pltpu.VMEM((7, tok_rows, LANES), jnp.float32),
        pltpu.VMEM((late, hidden), jnp.bfloat16), pltpu.VMEM((tok_rows, hidden), jnp.bfloat16),
        pltpu.VMEM((late, width // sides), jnp.bfloat16), dense, dense,
        semaphores((8,)), semaphores((2,)), one, semaphores((groups,)), one, one,
        semaphores((sides + 1,)), semaphores((sides + 1,)),
        semaphores((4,)), semaphores((2, 2, groups)), one,
        semaphores((5,)), semaphores((2, sides)), semaphores((sides,)),
        one, semaphores((2,)), one, one, pltpu.SemaphoreType.REGULAR((2,)),
    ]


def direct_scratch(tok_rows, width, hidden, buffer, sems):
    return [
        pltpu.VMEM((tok_rows, width), jnp.bfloat16),
        pltpu.VMEM((width, hidden), jnp.bfloat16),
        pltpu.VMEM((width, hidden), jnp.bfloat16),
        pltpu.VMEM((hidden, width), jnp.bfloat16),
        pltpu.VMEM((tok_rows, width), jnp.bfloat16),
        pltpu.VMEM((tok_rows, width), jnp.float32),
        pltpu.VMEM((LANES, tok_rows), jnp.float32),
        pltpu.VMEM((tok_rows, LANES), jnp.float32),
        pltpu.VMEM((tok_rows, LANES), jnp.float32),
        buffer,
        buffer,
        buffer,
        buffer,
        pltpu.SemaphoreType.DMA((4,)),
        sems,
        sems,
        sems,
        sems,
    ]


def shards(
    tokens, modality, expert_ids, route_weights, norm_gain, gate_weight, up_weight, down_weight
):
    devices = lax.axis_size(AXIS)
    tok_rows, width = tokens.shape
    fanout = expert_ids.shape[1]
    hidden = gate_weight.shape[1]
    capacity = min(tok_rows, tok_rows * fanout * 5 // (4 * devices))
    waves = 2 if capacity % 32 == 0 and capacity >= 256 else 1
    chunk = capacity // waves
    buffer = pltpu.VMEM((waves, devices, chunk, width), jnp.bfloat16)
    near = pl.BlockSpec(memory_space=pltpu.VMEM)
    far = pl.BlockSpec(memory_space=pl.ANY)
    sems = pltpu.SemaphoreType.DMA((waves, devices))
    blocks, groups, sides = 8, 4, 4
    paired = (
        devices == 4
        and lax.axis_size("dp") % 8 == 0
        and tok_rows % (LANES * groups) == 0
        and tok_rows % (64 * blocks) == 0
        and width % (64 * groups) == 0
        and width % (LANES * sides) == 0
        and hidden % 128 == 0
    )
    if paired:
        kernel = functools.partial(pair_kernel, blocks, groups, sides)
        scratch = pair_scratch(tok_rows, width, hidden, fanout, capacity, blocks, groups, sides)
    else:
        kernel = functools.partial(moe_kernel, devices)
        scratch = direct_scratch(tok_rows, width, hidden, buffer, sems)
    return pl.pallas_call(
        kernel,
        out_shape=pltpu.VMEM((tok_rows, width), jnp.bfloat16),
        in_specs=[far] + [far if paired else near] * 4 + [far] * 3,
        out_specs=near,
        scratch_shapes=scratch,
        compiler_params=pltpu.CompilerParams(
            collective_id=0, has_side_effects=True, vmem_limit_bytes=(60 if paired else 58) * 1024 * 1024
        ),
    )(
        tokens,
        modality.reshape(1, tok_rows),
        expert_ids.T,
        route_weights.T,
        norm_gain,
        gate_weight,
        up_weight,
        down_weight,
    )


def solution(mesh):
    placed = (
        P(("dp", AXIS), None),
        P(("dp", AXIS)),
        P(("dp", AXIS), None),
        P(("dp", AXIS), None),
        P(),
        P(None, AXIS),
        P(None, AXIS),
        P(AXIS, None),
    )
    return jax.shard_map(
        shards, mesh=mesh, in_specs=placed, out_specs=P(("dp", AXIS), None), check_vma=False
    )
```

```python
import functools

import jax
import jax.numpy as jnp
from jax import lax
from jax.experimental import pallas as pl
from jax.experimental.pallas import tpu as pltpu
from jax.sharding import PartitionSpec as P

epsilon = 1e-05
LANES = 128
AXIS = "expert"


def grid_side(devices):
    side = 1
    while side * side < devices:
        side += 1
    return side if side * side == devices else devices


def moe_kernel(
    devices,
    tokens_hbm,
    modality_ref,
    ids_ref,
    weights_ref,
    gain_ref,
    gate_hbm,
    up_hbm,
    down_hbm,
    out_ref,
    tokens,
    gate,
    up,
    down,
    normed,
    total,
    place_rows,
    place_cols,
    share_cols,
    packed,
    arrived,
    finished,
    returned,
    load_sem,
    go_send,
    go_recv,
    back_send,
    back_recv,
):
    waves, _, chunk, width = packed.shape
    tok_rows = tokens.shape[0]
    fanout = ids_ref.shape[0]
    me = lax.axis_index(AXIS)
    side = grid_side(devices)
    mine_hi, mine_lo = me // side, me % side
    lines = devices // side

    def ahead(step):
        return ((mine_hi + step // side) % lines) * side + (mine_lo + step % side) % side

    def behind(step):
        return ((mine_hi + lines - step // side) % lines) * side + (
            mine_lo + side - step % side
        ) % side

    def go(wave, step):
        return pltpu.make_async_remote_copy(
            src_ref=packed.at[wave, step],
            dst_ref=arrived.at[wave, step],
            send_sem=go_send.at[wave, step],
            recv_sem=go_recv.at[wave, step],
            device_id={AXIS: ahead(step)},
            device_id_type=pl.DeviceIdType.MESH,
        )

    def back(wave, step):
        return pltpu.make_async_remote_copy(
            src_ref=finished.at[wave, step],
            dst_ref=returned.at[wave, step],
            send_sem=back_send.at[wave, step],
            recv_sem=back_recv.at[wave, step],
            device_id={AXIS: behind(step)},
            device_id_type=pl.DeviceIdType.MESH,
        )

    loads = [
        pltpu.make_async_copy(tokens_hbm, tokens, load_sem.at[0]),
        pltpu.make_async_copy(gate_hbm, gate, load_sem.at[1]),
        pltpu.make_async_copy(up_hbm, up, load_sem.at[2]),
        pltpu.make_async_copy(down_hbm, down, load_sem.at[3]),
    ]
    for load in loads:
        load.start()

    barrier = pltpu.get_barrier_semaphore()

    def greet(step, carry):
        pl.semaphore_signal(
            barrier, inc=1, device_id={AXIS: ahead(step)}, device_id_type=pl.DeviceIdType.MESH
        )
        return carry

    lax.fori_loop(1, devices, greet, 0)

    expert = lax.broadcasted_iota(jnp.int32, (LANES, tok_rows), 0)
    named = jnp.zeros((LANES, tok_rows), jnp.float32)
    share = jnp.zeros((LANES, tok_rows), jnp.float32)
    for k in range(fanout):
        hit = expert == ids_ref[k : k + 1, :]
        named = jnp.where(hit, 1.0, named)
        share = jnp.where(hit, weights_ref[k : k + 1, :], share)
    before = (
        lax.broadcasted_iota(jnp.int32, (tok_rows, tok_rows), 0)
        < lax.broadcasted_iota(jnp.int32, (tok_rows, tok_rows), 1)
    )
    count = jnp.dot(
        named.astype(jnp.bfloat16),
        jnp.where(before, 1.0, 0.0).astype(jnp.bfloat16),
        preferred_element_type=jnp.float32,
    )
    place = jnp.where(named > 0.5, count, -1.0)
    place_rows[...] = place
    place_cols[...] = place.T
    share_cols[...] = share.T
    image = jnp.broadcast_to(modality_ref[...].astype(jnp.float32), (LANES, tok_rows)).T

    loads[0].wait()
    rows = 64
    for start in range(0, tok_rows, rows):
        values = tokens[start : start + rows, :].astype(jnp.float32)
        square = jnp.mean(values * values, axis=1, keepdims=True)
        gains = jnp.where(
            image[start : start + rows, :1] > 0.5, gain_ref[1:2, :], gain_ref[0:1, :]
        )
        normed[start : start + rows, :] = (
            values * lax.rsqrt(square + epsilon) * gains
        ).astype(jnp.bfloat16)

    def pack(wave, step, target):
        line = place_rows[pl.ds(ahead(step), 1), :]
        slot = lax.broadcasted_iota(jnp.int32, (chunk, tok_rows), 0) + wave * chunk
        pick = jnp.where(line == slot.astype(jnp.float32), 1.0, 0.0).astype(jnp.bfloat16)
        target[wave, step] = jnp.dot(
            pick, normed[...], preferred_element_type=jnp.float32
        ).astype(jnp.bfloat16)

    others = devices - 1
    items = waves * others

    def which(item):
        return item // others, others - item % others

    pl.semaphore_wait(barrier, others)

    def send(item, carry):
        wave, step = which(item)
        pack(wave, step, packed)
        go(wave, step).start()
        return carry

    lax.fori_loop(0, items, send, 0)

    for load in loads[1:]:
        load.wait()

    def feed(source, target, wave, step):
        value = source[wave, step]
        opened = jnp.dot(value, gate[...], preferred_element_type=jnp.float32)
        upper = jnp.dot(value, up[...], preferred_element_type=jnp.float32)
        active = (opened / (1.0 + jnp.exp(-opened)) * upper).astype(jnp.bfloat16)
        target[wave, step] = jnp.dot(
            active, down[...], preferred_element_type=jnp.float32
        ).astype(jnp.bfloat16)

    def spread(wave, step):
        lane = lax.broadcasted_iota(jnp.int32, (tok_rows, LANES), 1) == ahead(step)
        line = jnp.sum(jnp.where(lane, place_cols[...], 0.0), axis=1, keepdims=True)
        worth = jnp.sum(jnp.where(lane, share_cols[...], 0.0), axis=1, keepdims=True)
        slot = lax.broadcasted_iota(jnp.int32, (tok_rows, chunk), 1) + wave * chunk
        spots = jnp.where(line == slot.astype(jnp.float32), worth, 0.0)
        high = spots.astype(jnp.bfloat16)
        low = (spots - high.astype(jnp.float32)).astype(jnp.bfloat16)
        value = returned[wave, step]
        return jnp.dot(high, value, preferred_element_type=jnp.float32) + jnp.dot(
            low, value, preferred_element_type=jnp.float32
        )

    total[...] = tokens[...].astype(jnp.float32)

    def local(wave, carry):
        pack(wave, 0, arrived)
        feed(arrived, returned, wave, 0)
        total[...] += spread(wave, 0)
        return carry

    lax.fori_loop(0, waves, local, 0)

    def serve(item, carry):
        wave, step = which(item)
        go(wave, step).wait_recv()
        feed(arrived, finished, wave, step)
        back(wave, step).start()
        return carry

    lax.fori_loop(0, items, serve, 0)

    def collect(item, carry):
        wave, step = which(item)
        back(wave, step).wait_recv()
        total[...] += spread(wave, step)
        return carry

    lax.fori_loop(0, items - 1, collect, 0)
    wave, step = which(items - 1)
    back(wave, step).wait_recv()
    out_ref[...] = (total[...] + spread(wave, step)).astype(out_ref.dtype)

    def settle(item, carry):
        wave, step = which(item)
        go(wave, step).wait_send()
        back(wave, step).wait_send()
        return carry

    lax.fori_loop(0, items, settle, 0)


def pair_kernel(
    blocks,
    groups,
    sides,
    tokens_hbm,
    modality_hbm,
    ids_hbm,
    weights_hbm,
    gain_hbm,
    gate_hbm,
    up_hbm,
    down_hbm,
    out_ref,
    modality_ref,
    ids_ref,
    weights_ref,
    gain_ref,
    tokens,
    sorted_tokens,
    near_tokens,
    gate,
    up,
    down,
    far_gate,
    far_up,
    far_down,
    normed,
    near_normed,
    total,
    near_total,
    facts,
    sorted_facts,
    near_facts,
    slots,
    earlier,
    columns,
    active,
    own_active,
    relayed,
    sum_out,
    sum_in,
    load_sem,
    facts_sem,
    dense_send,
    dense_recv,
    sum_send,
    sum_recv,
    late_send,
    late_recv,
    wide_send,
    wide_recv,
    wide_join,
    tall_send,
    tall_recv,
    tall_join,
    out_send,
    out_recv,
    home_send,
    home_recv,
    entered,
):
    tok_rows, width = tokens.shape
    hidden = gate.shape[1]
    fanout = ids_ref.shape[0]
    devices = lax.axis_size(AXIS)
    capacity = tok_rows * fanout * 5 // (4 * devices)
    part = tok_rows // blocks
    free = (tok_rows - capacity) // part
    me = lax.axis_index(AXIS)
    copy_of = lax.axis_index("dp")
    layer, core = copy_of // 2, copy_of % 2
    beside = me // 2 * 2 + 1 - me % 2
    above = (1 - me // 2) * 2 + me % 2
    kind_of = layer // 2 % 2
    first = beside * (1 - kind_of) + above * kind_of
    second = above * (1 - kind_of) + beside * kind_of
    diagonal = (1 - me // 2) * 2 + 1 - me % 2
    other_layer = (layer // 2 * 2 + 1 - layer % 2) * 2 + core
    other_core = layer * 2 + 1 - core
    beside_layers = 1 + (layer % 4 + 1) // 2 % 2
    middle = beside_layers == 2
    across_layer = (layer // 4 * 4 + 3 - layer % 4) * 2 + core
    far_layer = (layer // 4 * 4 + (layer + 2) % 4) * 2 + core
    quarter = layer % 2 * 2 + core
    layer_quarter = (1 - layer % 2) * 2 + core

    def remote(source, target, send_sem, recv_sem, copy, peer):
        return pltpu.make_async_remote_copy(
            src_ref=source,
            dst_ref=target,
            send_sem=send_sem,
            recv_sem=recv_sem,
            device_id={"dp": copy, AXIS: peer},
            device_id_type=pl.DeviceIdType.MESH,
        )

    def part_rows(block):
        return pl.ds(pl.multiple_of(block * part, part), part)

    share_of = blocks // groups
    batch = tok_rows // groups

    def batch_rows(group):
        return pl.ds(pl.multiple_of(group * batch, batch), batch)

    def dense_rows(rows, group):
        return remote(
            sorted_tokens.at[rows],
            near_tokens.at[rows],
            dense_send,
            dense_recv.at[group],
            copy_of,
            first,
        )

    def dense(block):
        return dense_rows(part_rows(block), block // share_of)

    def sums_rows(rows):
        return remote(sum_out.at[rows], sum_in.at[rows], sum_send, sum_recv, copy_of, first)

    def sums(block):
        return sums_rows(part_rows(block))

    slim = width // sides

    def columns_of(side):
        return pl.ds(side * slim, slim)

    detours = blocks - free - 1

    def late_rows(index):
        begin = {0: free + detours, sides: blocks - 1}.get(index, free)
        end = blocks - 1 if index == sides - 1 else blocks
        return pl.ds(begin * part, (end - begin) * part)

    def late_sums(index):
        spot = (late_rows(index), columns_of(min(index, sides - 1)))
        return remote(
            sum_out.at[spot],
            sum_in.at[spot],
            late_send.at[index],
            late_recv.at[index],
            copy_of,
            first,
        )

    def out_rows(begin, end, which):
        rows = pl.ds(begin * part, (end - begin) * part)
        return remote(
            sum_out.at[pl.ds((free + begin) * part, (end - begin) * part), columns_of(0)],
            relayed.at[rows],
            out_send,
            out_recv.at[which],
            far_layer,
            first,
        )

    def home_rows(begin, end):
        return remote(
            relayed.at[pl.ds(begin * part, (end - begin) * part)],
            sum_in.at[pl.ds((free + begin) * part, (end - begin) * part), columns_of(0)],
            home_send,
            home_recv,
            far_layer,
            me,
        )

    cut = detours // 2
    spans = tuple((begin, begin + 1) for begin in range(detours))

    wide_rows = width // 4 // groups
    tall_rows = hidden // 4

    def weight_copy(stage, kind, index):
        which = layer_quarter if stage in (3, 4) else quarter
        if kind < 2:
            near, far = ((gate_hbm, far_gate), (up_hbm, far_up))[kind]
            send = wide_send.at[stage]
            recv = wide_join if stage in (2, 3) else wide_recv.at[kind, stage, index]
            start = which * (width // 4) + index * wide_rows
            spot = (pl.ds(pl.multiple_of(start, wide_rows), wide_rows),)
        else:
            near, far, send = down_hbm, far_down, tall_send.at[stage]
            recv = tall_join.at[index] if stage in (2, 3) else tall_recv.at[stage % 3, index]
            start = which * tall_rows
            spot = (pl.ds(pl.multiple_of(start, tall_rows), tall_rows), columns_of(index))
        return weight_remote(
            stage, (near if stage in (0, 4) else far).at[spot], far.at[spot], send, recv
        )

    def weight_remote(stage, source, target, send, recv):
        copy, peer = (
            (copy_of, second),
            (other_layer, me),
            (other_core, me),
            (other_core, me),
            (copy_of, second),
        )[stage]
        return remote(source, target, send, recv, copy, peer)

    def wide_joined():
        weight_remote(2, far_gate, far_gate, wide_send.at[2], wide_join).wait_recv()

    def tall_joined(side):
        both = far_down.at[pl.ds(0, 2 * tall_rows), columns_of(side)]
        weight_remote(2, both, both, tall_send.at[2], tall_join.at[side]).wait_recv()

    def weights_sent():
        wide = far_gate.at[pl.ds(0, width // 2)]
        for stage in range(4):
            weight_remote(stage, wide, wide, wide_send.at[stage], wide_join).wait_send()
        for stage, wholes in enumerate((sides, sides - 1, sides, sides, 1)):
            tall = far_down.at[pl.ds(0, tall_rows), pl.ds(0, wholes * slim)]
            weight_remote(stage, tall, tall, tall_send.at[stage], tall_join.at[0]).wait_send()

    def arrived_across(kind, index):
        weight_copy(0, kind, index).wait_recv()
        if kind < 2 or index < sides - 1:
            weight_copy(1, kind, index).start()
        weight_copy(2, kind, index).start()

    def arrived_along(kind, index):
        weight_copy(1 if kind < 2 or index < sides - 1 else 4, kind, index).wait_recv()
        weight_copy(3, kind, index).start()

    def each(count, step, start=0):
        def body(index, carry):
            step(index)
            return carry

        lax.fori_loop(start, count, body, 0)

    loads = [
        pltpu.make_async_copy(source, target, load_sem.at[index])
        for index, (source, target) in enumerate(
            (
                (ids_hbm, ids_ref),
                (weights_hbm, weights_ref),
                (modality_hbm, modality_ref),
                (tokens_hbm, tokens),
                (gain_hbm, gain_ref),
                (gate_hbm, gate),
                (up_hbm, up),
                (down_hbm, down),
            )
        )
    ]
    barrier = pltpu.get_barrier_semaphore()
    partners = (
        (copy_of, first),
        (copy_of, second),
        (other_layer, me),
        (other_core, me),
    )

    def tell(semaphore, copy, peer):
        pl.semaphore_signal(
            semaphore,
            inc=1,
            device_id={"dp": copy, AXIS: peer},
            device_id_type=pl.DeviceIdType.MESH,
        )

    def along_line(step):
        step(other_layer)

        @pl.when(middle)
        def _():
            step(across_layer)

    for copy, peer in partners:
        tell(barrier, copy, peer)

    @pl.when(middle)
    def _():
        tell(barrier, across_layer, me)

    for load in loads[:5]:
        load.start()
    earlier[...] = jnp.where(
        lax.broadcasted_iota(jnp.int32, (tok_rows, tok_rows), 0)
        < lax.broadcasted_iota(jnp.int32, (tok_rows, tok_rows), 1),
        1.0,
        0.0,
    ).astype(jnp.bfloat16)
    lines = 8
    expert = lax.broadcasted_iota(jnp.int32, (lines, tok_rows), 0)
    loads[0].wait()
    late_ones = jnp.zeros((1, tok_rows), jnp.float32)
    for k in range(fanout):
        late_ones = jnp.where(ids_ref[k : k + 1, :] == diagonal, 1.0, late_ones)
    named = jnp.where(expert == 0, late_ones, 1.0 - late_ones)
    count = jnp.dot(
        named.astype(jnp.bfloat16), earlier[...], preferred_element_type=jnp.float32
    )
    slots[...] = jnp.broadcast_to(
        jnp.where(late_ones > 0.5, tok_rows - 1.0 - count[0:1, :], count[1:2, :]),
        (lines, tok_rows),
    )

    def sort(block):
        slot = lax.broadcasted_iota(jnp.int32, (part, tok_rows), 0) + block * part
        pick = jnp.where(slots[0:1, :] == slot.astype(jnp.float32), 1.0, 0.0).astype(jnp.bfloat16)
        sorted_tokens[part_rows(block)] = jnp.dot(
            pick, tokens[...], preferred_element_type=jnp.float32
        ).astype(jnp.bfloat16)

    loads[3].wait()
    sort(0)
    pl.semaphore_wait(barrier, len(partners) - 1 + beside_layers)

    dense(0).start()
    sort(1)
    dense(1).start()
    along_line(lambda copy: tell(entered.at[0], copy, me))
    each(groups, lambda index: [weight_copy(0, kind, index).start() for kind in range(2)])
    for side in range(sides):
        weight_copy(0, 2, side).start()
    weight_copy(4, 2, sides - 1).start()

    for load in loads[5:]:
        load.start()
    for load in loads[1:3]:
        load.wait()
    share = jnp.where(
        expert == devices,
        jnp.broadcast_to(modality_ref[...].astype(jnp.float32), (lines, tok_rows)),
        0.0,
    )
    for k in range(fanout):
        share = jnp.where(expert == ids_ref[k : k + 1, :], weights_ref[k : k + 1, :], share)
    facts[...] = share

    def keep(place, line):
        columns[place] = jnp.broadcast_to(line, (LANES, tok_rows)).T

    own_mine, own_far, near_mine, near_far, near_image, own_image, own_slot = range(7)
    keep(own_slot, slots[0:1, :])
    keep(own_mine, facts[pl.ds(me, 1), :])
    keep(own_far, facts[pl.ds(second, 1), :])
    keep(own_image, facts[devices : devices + 1, :])

    def places(start, count):
        slot = lax.broadcasted_iota(jnp.int32, (tok_rows, count), 1) + start
        here = columns[own_slot, :, 0:1] == slot.astype(jnp.float32)
        return jnp.where(here, 1.0, 0.0).astype(jnp.bfloat16)

    coarse = share.astype(jnp.bfloat16)
    fine = (share - coarse.astype(jnp.float32)).astype(jnp.bfloat16)
    every = places(0, tok_rows)
    sorted_facts[...] = jnp.dot(coarse, every, preferred_element_type=jnp.float32) + jnp.dot(
        fine, every, preferred_element_type=jnp.float32
    )
    told = remote(sorted_facts, near_facts, facts_sem.at[0], facts_sem.at[1], copy_of, first)
    told.start()

    def leave(block):
        sort(block)
        dense(block).start()

    each(blocks, leave, 2)

    def normalize(source, target, image, rows):
        values = source[rows, :].astype(jnp.float32)
        square = jnp.mean(values * values, axis=1, keepdims=True)
        gains = jnp.where(image > 0.5, gain_ref[1:2, :], gain_ref[0:1, :])
        target[rows, :] = (values * lax.rsqrt(square + epsilon) * gains).astype(jnp.bfloat16)

    def activate(value, opening, upping):
        opened = jnp.dot(value, opening[...], preferred_element_type=jnp.float32)
        upper = jnp.dot(value, upping[...], preferred_element_type=jnp.float32)
        return (opened / (1.0 + jnp.exp(-opened)) * upper).astype(jnp.bfloat16)

    def settle(value, closing):
        result = jnp.dot(value, closing, preferred_element_type=jnp.float32)
        return result.astype(jnp.bfloat16).astype(jnp.float32)

    def feed(value, opening, upping, closing):
        return settle(activate(value, opening, upping), closing[...])

    loads[4].wait()
    rows = 64

    def ready(index):
        here = pl.ds(pl.multiple_of(index * rows, rows), rows)
        normalize(tokens, normed, columns[own_image, here, 0:1], here)

    each(tok_rows // rows, ready)
    pl.semaphore_wait(entered.at[0], beside_layers)
    along_line(lambda copy: tell(entered.at[1], copy, me))
    for load in loads[5:]:
        load.wait()

    double = 2 * batch

    def pair_rows(group):
        return pl.ds(pl.multiple_of(group * double, double), double)

    def both(group):
        arrived_across(0, group)

        @pl.when(group < tok_rows // double)
        def _():
            here = pair_rows(group)
            total[here, :] = tokens[here, :].astype(jnp.float32) + columns[
                own_mine, here, 0:1
            ] * feed(normed[here, :], gate, up, down)

        @pl.when(group > 0)
        def _():
            arrived_along(1, group - 1)

        arrived_across(1, group)

        @pl.when(group == 0)
        def _():
            told.wait_recv()
            keep(near_mine, near_facts[pl.ds(me, 1), :])
            keep(near_far, near_facts[pl.ds(second, 1), :])
            keep(near_image, near_facts[devices : devices + 1, :])

        @pl.when(group == groups - 1)
        def _():
            arrived_across(2, 0)

        here = batch_rows(group)
        dense_rows(here, group).wait_recv()
        for start in range(0, batch, rows):
            few = pl.ds(pl.multiple_of(group * batch + start, rows), rows)
            normalize(near_tokens, near_normed, columns[near_image, few, 0:1], few)
        near = columns[near_mine, here, 0:1] * feed(near_normed[here, :], gate, up, down)
        near_total[here, :] = near
        sum_out[here, :] = near.astype(jnp.bfloat16)
        for index in range(share_of):
            block = group * share_of + index

            @pl.when(block < free)
            def _():
                sums(block).start()

        arrived_along(0, group)

    each(groups, both)
    arrived_along(1, groups - 1)
    arrived_across(2, 1)

    late = slice(free * part, tok_rows)
    wide_joined()
    active[...] = activate(near_normed[late, :], far_gate, far_up)

    def finish(side):
        tall_joined(side)
        there = slice(side * slim, (side + 1) * slim)
        sum_out[late, there] = (
            near_total[late, there]
            + columns[near_far, late, 0:1] * settle(active[...], far_down[:, there])
        ).astype(jnp.bfloat16)
        if side == 0:
            for which, (begin, end) in enumerate(spans):
                out_rows(begin, end, which).start()
        late_sums(side).start()
        if side == sides - 1:
            late_sums(sides).start()

    def pass_on(which):
        begin, end = spans[which]
        out_rows(begin, end, which).wait_recv()
        home_rows(begin, end).start()

    def own(group):
        here = pair_rows(group)
        own_active[here, :] = activate(normed[here, :], far_gate, far_up)

    def own_finish(side):
        there = slice(side * slim, (side + 1) * slim)
        total[:, there] += columns[own_far, :, 0:1] * settle(own_active[...], far_down[:, there])

    pl.semaphore_wait(entered.at[1], beside_layers)
    arrived_along(2, 0)
    finish(0)
    arrived_across(2, 2)
    arrived_along(2, 1)
    finish(1)
    own(0)
    arrived_across(2, 3)
    arrived_along(2, 2)
    finish(2)
    for which in range(cut):
        pass_on(which)
    each(tok_rows // double, own, 1)
    arrived_along(2, 3)
    finish(3)
    for which in range(cut, detours):
        pass_on(which)
    sums_rows(pl.ds(0, free * part)).wait_recv()
    total[...] += jnp.dot(
        places(0, free * part), sum_in[: free * part, :], preferred_element_type=jnp.float32
    )
    for side in range(sides):
        own_finish(side)

    def gathered(side, begin, end):
        return total[:, side * slim : (side + 1) * slim] + jnp.dot(
            places(begin * part, (end - begin) * part),
            sum_in[begin * part : end * part, side * slim : (side + 1) * slim],
            preferred_element_type=jnp.float32,
        )

    def take(side):
        out_ref[:, side * slim : (side + 1) * slim] = gathered(side, free, blocks).astype(
            out_ref.dtype
        )

    for side in range(1, sides - 1):
        late_sums(side).wait_recv()
        take(side)
    home_rows(0, detours).wait_recv()
    late_sums(0).wait_recv()
    take(0)
    told.wait_send()
    dense_rows(pl.ds(0, tok_rows), 0).wait_send()
    sums_rows(pl.ds(0, free * part)).wait_send()
    for side in range(sides - 1):
        late_sums(side).wait_send()
    out_rows(0, detours, 0).wait_send()
    home_rows(0, detours).wait_send()
    weights_sent()

    side = sides - 1
    there = slice(side * slim, width)
    late_sums(side).wait_recv()
    total[:, there] = gathered(side, free, blocks - 1)
    late_sums(sides).wait_recv()
    out_ref[:, there] = gathered(side, blocks - 1, blocks).astype(out_ref.dtype)
    late_sums(side).wait_send()
    late_sums(sides).wait_send()


def pair_scratch(tok_rows, width, hidden, fanout, capacity, blocks, groups, sides):
    dense = pltpu.VMEM((tok_rows, width), jnp.bfloat16)
    sums = pltpu.VMEM((tok_rows, width), jnp.float32)
    facts = pltpu.VMEM((8, tok_rows), jnp.float32)
    wide = pltpu.VMEM((width, hidden), jnp.bfloat16)
    tall = pltpu.VMEM((hidden, width), jnp.bfloat16)
    semaphores = pltpu.SemaphoreType.DMA
    one = semaphores(())
    part = tok_rows // blocks
    late = tok_rows - (tok_rows - capacity) // part * part
    return [
        pltpu.VMEM((1, tok_rows), jnp.int32), pltpu.VMEM((fanout, tok_rows), jnp.int32),
        pltpu.VMEM((fanout, tok_rows), jnp.float32), pltpu.VMEM((2, width), jnp.float32),
        dense, dense, dense, wide, wide, tall, wide, wide, tall, dense, dense, sums, sums,
        facts, facts, facts, facts, pltpu.VMEM((tok_rows, tok_rows), jnp.bfloat16),
        pltpu.VMEM((7, tok_rows, LANES), jnp.float32),
        pltpu.VMEM((late, hidden), jnp.bfloat16), pltpu.VMEM((tok_rows, hidden), jnp.bfloat16),
        pltpu.VMEM((late, width // sides), jnp.bfloat16), dense, dense,
        semaphores((8,)), semaphores((2,)), one, semaphores((groups,)), one, one,
        semaphores((sides + 1,)), semaphores((sides + 1,)),
        semaphores((4,)), semaphores((2, 2, groups)), one,
        semaphores((5,)), semaphores((2, sides)), semaphores((sides,)),
        one, semaphores((late // part - 1,)), one, one, pltpu.SemaphoreType.REGULAR((2,)),
    ]


def direct_scratch(tok_rows, width, hidden, buffer, sems):
    return [
        pltpu.VMEM((tok_rows, width), jnp.bfloat16),
        pltpu.VMEM((width, hidden), jnp.bfloat16),
        pltpu.VMEM((width, hidden), jnp.bfloat16),
        pltpu.VMEM((hidden, width), jnp.bfloat16),
        pltpu.VMEM((tok_rows, width), jnp.bfloat16),
        pltpu.VMEM((tok_rows, width), jnp.float32),
        pltpu.VMEM((LANES, tok_rows), jnp.float32),
        pltpu.VMEM((tok_rows, LANES), jnp.float32),
        pltpu.VMEM((tok_rows, LANES), jnp.float32),
        buffer,
        buffer,
        buffer,
        buffer,
        pltpu.SemaphoreType.DMA((4,)),
        sems,
        sems,
        sems,
        sems,
    ]


def shards(
    tokens, modality, expert_ids, route_weights, norm_gain, gate_weight, up_weight, down_weight
):
    devices = lax.axis_size(AXIS)
    tok_rows, width = tokens.shape
    fanout = expert_ids.shape[1]
    hidden = gate_weight.shape[1]
    capacity = min(tok_rows, tok_rows * fanout * 5 // (4 * devices))
    waves = 2 if capacity % 32 == 0 and capacity >= 256 else 1
    chunk = capacity // waves
    buffer = pltpu.VMEM((waves, devices, chunk, width), jnp.bfloat16)
    near = pl.BlockSpec(memory_space=pltpu.VMEM)
    far = pl.BlockSpec(memory_space=pl.ANY)
    sems = pltpu.SemaphoreType.DMA((waves, devices))
    blocks, groups, sides = 8, 4, 4
    paired = (
        devices == 4
        and fanout == 2
        and lax.axis_size("dp") % 8 == 0
        and tok_rows % (LANES * groups) == 0
        and tok_rows % (64 * blocks) == 0
        and width % (64 * groups) == 0
        and width % (LANES * sides) == 0
        and hidden % 128 == 0
    )
    if paired:
        kernel = functools.partial(pair_kernel, blocks, groups, sides)
        scratch = pair_scratch(tok_rows, width, hidden, fanout, capacity, blocks, groups, sides)
    else:
        kernel = functools.partial(moe_kernel, devices)
        scratch = direct_scratch(tok_rows, width, hidden, buffer, sems)
    return pl.pallas_call(
        kernel,
        out_shape=pltpu.VMEM((tok_rows, width), jnp.bfloat16),
        in_specs=[far] + [far if paired else near] * 4 + [far] * 3,
        out_specs=near,
        scratch_shapes=scratch,
        compiler_params=pltpu.CompilerParams(
            collective_id=0, has_side_effects=True, vmem_limit_bytes=(60 if paired else 58) * 1024 * 1024
        ),
    )(
        tokens,
        modality.reshape(1, tok_rows),
        expert_ids.T,
        route_weights.T,
        norm_gain,
        gate_weight,
        up_weight,
        down_weight,
    )


def solution(mesh):
    placed = (
        P(("dp", AXIS), None),
        P(("dp", AXIS)),
        P(("dp", AXIS), None),
        P(("dp", AXIS), None),
        P(),
        P(None, AXIS),
        P(None, AXIS),
        P(AXIS, None),
    )
    return jax.shard_map(
        shards, mesh=mesh, in_specs=placed, out_specs=P(("dp", AXIS), None), check_vma=False
    )
```
